32 devices in a mesh: gossip: 16 (over z, y, core), mp: 2 (over x).
Axes of the slice: x: 2, y: 2, z: 4, core: 2. Of those that a mesh axis runs over, the one named last changes fastest.
Arguments:
- params: float32 [16, 1024, 4096], P('gossip', None, 'mp'), may hold values from -6 to 6
- public: float32 [16, 1024, 64], P('gossip'), may hold values from -12 to 12
- gradients: bfloat16 [2, 16, 1024, 4096], P(None, 'gossip', None, 'mp'), may hold values from -130 to 130
- projection: float32 [4096, 64], P('mp'), may hold values from -0.09375 to 0.09375
- partners: int32 [2, 16], P(None, 'gossip'), may hold values from 0 to 15, as said below
Outputs:
- params_out: float32 [16, 1024, 4096], P('gossip', None, 'mp')
- public_out: float32 [16, 1024, 64], P('gossip')
- consensus: float32 [2], replicated
- grad_norm: float32 [2], replicated
The draws below stay inside these ranges and needn't reach their ends.
Inputs may be any that keep to these rules, and one draw needn't show every extreme that they name: Each row is a pairing of the 16 replicas: partners[r, partners[r, i]] = i and partners[r, i] != i.
All inputs are finite; a program needn't handle non-finite values.
Results may differ from the reference program's by a relative error of at most 0.008.
Values may be sent and summed in bfloat16 or wider, within the bound.
A program may use at most 64 MiB of HBM per device.

```python
import math
import jax
import jax.numpy as jnp
from jax import lax

SLAB = 4096
RANK = 64
ROWS = 1024
ROUNDS = 2
NODES = 16


def draw_gradients(key, part):
    keys = jax.random.split(key, 5)
    shape = (ROUNDS, NODES, ROWS, SLAB)
    row_scale = jnp.exp(jax.random.uniform(keys[0], (ROUNDS, NODES, ROWS, 1), jnp.float32, math.log(0.3), math.log(3.0)))
    col_scale = jnp.exp(jax.random.uniform(keys[1], (ROUNDS, 1, 1, SLAB), jnp.float32, math.log(0.3), math.log(3.0)))
    node_scale = jnp.exp(jnp.linspace(0.0, math.log(3.0), NODES)).reshape(1, NODES, 1, 1)
    base = jnp.clip(jax.random.normal(keys[4], shape, jnp.float32), -4.0, 4.0)
    return (base * row_scale * col_scale * node_scale).astype(jnp.bfloat16)


def draw_public(key, part):
    keys = jax.random.split(key, 3)
    shape = (NODES, ROWS, RANK)
    node_scale = jnp.exp(jnp.linspace(0.0, math.log(3.0), NODES)).reshape(NODES, 1, 1)
    base = jnp.clip(jax.random.normal(keys[2], shape, jnp.float32), -4.0, 4.0)
    return (base * node_scale).astype(jnp.float32)


def draw_partners(key, part):
    rows_list = []
    for round_index in range(ROUNDS):
        order = jax.random.permutation(jax.random.fold_in(key, 71 + round_index), NODES).astype(jnp.int32)
        first = order[0::2]
        second = order[1::2]
        paired = jnp.zeros((NODES,), jnp.int32).at[first].set(second).at[second].set(first)
        rows_list.append(paired)
    return jnp.stack(rows_list)


def steps_of(key, dims, pieces, least, high):
    factor_of = 1.0
    for axis_at, blocks in pieces:
        draws = jax.random.uniform(jax.random.fold_in(jax.random.fold_in(key, 6), axis_at), (blocks,), jnp.float32, least / len(pieces), high / len(pieces))
        factor_of = factor_of * jnp.repeat(jnp.exp(draws), dims[axis_at] // blocks).reshape((-1,) + (1,) * (len(dims) - 1 - axis_at))
    return factor_of


def normal_values(own_key, dims, deviation, reach, cuts=(), kind=jnp.bfloat16):
    drawn = jax.random.normal(own_key, dims, jnp.float32) * deviation
    if len(cuts) > 0:
        drawn = steps_of(own_key, dims, cuts, -0.22, 0.18) * drawn
    return jnp.clip(drawn, min=-reach, max=reach).astype(kind)


def setup_inputs(seed: int = 0) -> dict:
    arg_keys = jax.random.split(jax.random.key(seed), 6)
    return {
        "params": normal_values(arg_keys[0], (NODES, ROWS, SLAB), 1.0, 6.0, ((0, 16), (2, 2)), jnp.float32),
        "public": draw_public(jax.random.fold_in(arg_keys[5], 71), 0),
        "gradients": draw_gradients(jax.random.fold_in(arg_keys[5], 71), 0),
        "projection": normal_values(arg_keys[3], (SLAB, RANK), SLAB ** -0.5, 0.09375, ((0, 2),), jnp.float32),
        "partners": draw_partners(jax.random.fold_in(arg_keys[5], 71), 0),
    }


step_size = 1.0
clip_limit = 0.5
mixing = 0.4
epsilon = 1e-06

def reference(params, public, gradients, projection, partners):
    highest = lax.Precision.HIGHEST
    total = NODES * ROWS * SLAB
    weights = params
    public_state = public
    drift_list = []
    norm_list = []
    for round_index in range(ROUNDS):
        grad_round = gradients[round_index]
        squares = jnp.sum(lax.map(lambda block: jnp.sum(jnp.square(block.astype(jnp.float32))), grad_round))
        norm_value = jnp.sqrt(squares / total + epsilon)
        scale = jnp.minimum(1.0, clip_limit / norm_value)

        def coefficients(item):
            node_weights, node_grad, node_coef = item
            half = node_weights - step_size * scale * node_grad.astype(jnp.float32)
            rebuilt = jnp.dot(node_coef, projection.T, precision=highest)
            return node_coef + jnp.dot(half - rebuilt, projection, precision=highest)
        coef = lax.map(coefficients, (weights, grad_round, public_state))
        sent = coef.astype(jnp.bfloat16)
        mate = jnp.take(sent, partners[round_index], axis=0)
        public_state = sent.astype(jnp.float32)

        def blend(item):
            node_weights, node_grad, own_coef, other_coef = item
            half = node_weights - step_size * scale * node_grad.astype(jnp.float32)
            drift = jnp.dot(other_coef.astype(jnp.float32) - own_coef, projection.T, precision=highest)
            return (half + mixing * drift, jnp.sum(drift * drift))
        weights, terms = lax.map(blend, (weights, grad_round, public_state, mate))
        drift_list.append(jnp.sum(terms) / total)
        norm_list.append(norm_value)
    return (weights, public_state, jnp.stack(drift_list), jnp.stack(norm_list))
```

```python
import functools

import jax
import jax.numpy as jnp
from jax import lax
from jax.experimental import pallas as pl
from jax.experimental.pallas import tpu as pltpu
from jax.sharding import PartitionSpec as P

ROUNDS = 2
step_size = 1.0
clip_limit = 0.5
mixing = 0.4
epsilon = 1e-06

F32 = jnp.float32
BF16 = jnp.bfloat16
VMEM = pl.BlockSpec(memory_space=pltpu.VMEM)
HBM = pl.BlockSpec(memory_space=pltpu.HBM)
ANYWHERE = pl.BlockSpec(memory_space=pl.ANY)
MESH = pl.DeviceIdType.MESH


def high_low(value):
    high = value.astype(BF16)
    return high, (value - high.astype(F32)).astype(BF16)


def dot(a, b):
    return jnp.dot(a, b, preferred_element_type=F32)


def dot_t(a, b):
    return lax.dot_general(a, b, (((1,), (1,)), ((), ())), preferred_element_type=F32)


def t_dot(a, b):
    return lax.dot_general(a, b, (((0,), (0,)), ((), ())), preferred_element_type=F32)


def each(low, high, act):
    lax.fori_loop(low, high, lambda i, _: (act(i), 0)[1], 0)


def exchange(groups, members, total, w_hbm, g_hbm, c_hbm, p_hbm, partners_hbm,
             half_ref, f_ref, basis, stat_ref,
             gv, cv, pv, partners_ref, squares, bd_own, a_own, extra, bd_send, bd_in, a_send, a_in, grams,
             norms, pairs, cons, owned, first, choose, apart_ref, reply, final,
             load_g, load_w, load_p, send_n, recv_n, send_t, recv_t, send_m, recv_m,
             send_u, recv_u, send_f, recv_f):
    g = lax.axis_index("gossip")
    m = lax.axis_index("mp")
    count = groups * members
    me = g * members + m
    phases, block, lanes = bd_own.shape
    subs = a_in.shape[2]
    step = block // subs
    steps = phases * members * subs
    rows = owned.shape[2]
    flat = groups * rows
    rank = lanes // 2
    columns = gv.shape[2]

    def span(i):
        j = i // subs
        q = lax.rem(m + j % members + 1, members)
        start = ((j // members) * members + q) * block + (i % subs) * step
        return pl.ds(pl.multiple_of(start, step), step)

    def grad_copy(i):
        return pltpu.make_async_copy(g_hbm.at[:, 0, span(i)], gv.at[:, span(i)], load_g.at[i])

    def weight_copy(i):
        return pltpu.make_async_copy(w_hbm.at[0, span(i)], half_ref.at[0, span(i)], load_w.at[i])

    basis_copy = pltpu.make_async_copy(p_hbm, pv, load_p.at[0])
    public_copy = pltpu.make_async_copy(c_hbm, cv, load_p.at[1])
    partners_copy = pltpu.make_async_copy(partners_hbm, partners_ref, load_p.at[2])
    basis_copy.start()
    partners_copy.start()
    each(0, steps, lambda i: grad_copy(i).start())

    def device(k):
        d = lax.rem(me + k, count)
        return d, d // members, d % members

    barrier = pltpu.get_barrier_semaphore()

    def greet(k):
        _, p, q = device(k)
        pl.semaphore_signal(barrier, inc=1, device_id={"gossip": p, "mp": q}, device_id_type=MESH)

    each(1, count, greet)

    def wide_copy(slot, ref, d, p, q, into):
        return pltpu.make_async_remote_copy(
            src_ref=ref.at[me], dst_ref=ref.at[into], send_sem=send_n.at[slot, d], recv_sem=recv_n.at[slot, into],
            device_id={"gossip": p, "mp": q}, device_id_type=MESH)

    def wide_start(slot, ref):
        def act(k):
            d, p, q = device(k)
            wide_copy(slot, ref, d, p, q, me).start()
        each(1, count, act)

    def wide_finish(slot, ref):
        def act(k):
            d, p, q = device(k)
            wide_copy(slot, ref, d, p, q, d).wait()
        each(1, count, act)

    def gossip_peers(act):
        each(1, groups, lambda k: act(lax.rem(g + k, groups)))

    def mp_peers(act):
        each(1, members, lambda k: act(lax.rem(m + k, members)))

    def pair_copy(p, into):
        return pltpu.make_async_remote_copy(
            src_ref=pairs.at[g], dst_ref=pairs.at[into], send_sem=send_t.at[phases, p], recv_sem=recv_t.at[phases, into],
            device_id={"gossip": p}, device_id_type=MESH)

    def piece_copy(h, p, into):
        return pltpu.make_async_remote_copy(
            src_ref=owned.at[h, p], dst_ref=first.at[h, into], send_sem=send_t.at[h, p], recv_sem=recv_t.at[h, into],
            device_id={"gossip": p}, device_id_type=MESH)

    def gram_copy(q, into):
        return pltpu.make_async_remote_copy(
            src_ref=grams.at[m], dst_ref=grams.at[into], send_sem=send_m.at[q], recv_sem=recv_m.at[into],
            device_id={"mp": q}, device_id_type=MESH)

    def bd_copy(h, q, into):
        return pltpu.make_async_remote_copy(
            src_ref=bd_send.at[h, q], dst_ref=bd_in.at[h, into], send_sem=send_u.at[0, h, q], recv_sem=recv_u.at[0, h, into],
            device_id={"mp": q}, device_id_type=MESH)

    def a_copy(h, q, into):
        return pltpu.make_async_remote_copy(
            src_ref=a_send.at[h, q], dst_ref=a_in.at[h, into], send_sem=send_u.at[1, h, q], recv_sem=recv_u.at[1, h, into],
            device_id={"mp": q}, device_id_type=MESH)

    def result_copy(h, k, from_device, from_p, from_q):
        d, p, q = device(k)
        return pltpu.make_async_remote_copy(
            src_ref=reply.at[h, p], dst_ref=final.at[h, from_q, from_p], send_sem=send_f.at[h, d],
            recv_sem=recv_f.at[h, from_device], device_id={"gossip": p, "mp": q}, device_id_type=MESH)

    squares[...] = jnp.zeros_like(squares)
    basis_copy.wait()
    high, low = high_low(pv[...])
    basis[...] = jnp.concatenate([high, low], axis=0)

    def fold(value):
        return value + pltpu.roll(value, rank, 1)

    def lower(value):
        return lax.broadcasted_iota(jnp.int32, value.shape, value.ndim - 1) < rank

    def place(i):
        j = i // subs
        return j // members, lax.rem(m + j % members + 1, members), pl.ds(pl.multiple_of((i % subs) * step, step), step)

    def grad_step(i):
        grad_copy(i).wait()
        weight_copy(i).start()
        products = []
        for index in range(ROUNDS):
            grad = gv[index, span(i)]
            wide = grad.astype(F32)
            squares[index] += jnp.sum((wide * wide).reshape(step // 8, 8, columns), axis=0)
            products.append(fold(dot_t(grad, basis[...])))
        h, q, inside = place(i)
        both = jnp.where(lower(products[0]), products[0], products[1])
        bd_own[h, inside] = both
        bd_send[h, q, inside] = both.astype(BF16)

    each(0, steps, grad_step)
    public_copy.start()
    partners_copy.wait()
    for index in range(ROUNDS):
        norms[me, index : index + 1] = jnp.full((1, lanes), jnp.sum(squares[index]), F32)
        pairs[g, index : index + 1] = jnp.full((1, lanes), partners_ref[index].astype(F32), F32)

    pl.semaphore_wait(barrier, count - 1)
    wide_start(0, norms)
    for h in range(phases):
        mp_peers(lambda q: bd_copy(h, q, m).start())

    parts = dot_t(basis[...], basis[...])
    folded = parts + pltpu.roll(parts, rank, 1)
    grams[m] = folded[:rank] + folded[rank:]
    mp_peers(lambda q: gram_copy(q, m).start())
    gossip_peers(lambda p: pair_copy(p, g).start())

    def weight_step(i):
        weight_copy(i).wait()
        high, low = high_low(half_ref[0, span(i)])
        product = fold(dot_t(high, basis[...]) + dot_t(low, basis[...]))
        h, q, inside = place(i)
        a_own[h, inside] = product
        packed = jnp.where(lower(product[: step // 2]), product[: step // 2], product[step // 2 :])
        a_send[h, q, i % subs] = packed.astype(BF16)

    def weight_block(j):
        each(0, subs, lambda s: weight_step(j * subs + s))

        @pl.when(j % members < members - 1)
        def _():
            a_copy(j // members, lax.rem(m + j % members + 1, members), m).start()

    each(0, phases * members, weight_block)

    mp_peers(lambda q: gram_copy(q, q).wait())
    gram = grams[0]
    for index in range(1, members):
        gram = gram + grams[index]
    gram_row = lax.broadcasted_iota(jnp.int32, gram.shape, 0)
    gram_lane = lax.broadcasted_iota(jnp.int32, gram.shape, 1)
    mixer_high, mixer_low = high_low(jnp.where(gram_lane < rank, jnp.where(gram_row == gram_lane, 1.0, 0.0) - gram, 0.0))
    public_copy.wait()
    for h in range(phases):
        at = pl.ds(pl.multiple_of((h * members + m) * block, block), block)
        high, low = high_low(cv[:, at])
        extra[h] = t_dot(high, mixer_high) + t_dot(low, mixer_high) + t_dot(high, mixer_low)

    wide_finish(0, norms)
    norm = jnp.sqrt(jnp.sum(norms[...], axis=0) / total + epsilon)
    scale = step_size * jnp.minimum(1.0, clip_limit / norm)
    scale_0 = scale[0:1]
    scale_1 = scale[1:2]

    for h in range(phases):
        def arrive(q):
            bd_copy(h, q, q).wait()
            a_copy(h, q, q).wait()
        mp_peers(arrive)
        both = bd_own[h]
        adds = [jnp.zeros((step // 2, lanes), F32) for _ in range(subs)]
        for index in range(1, members):
            q = lax.rem(m + index, members)
            both = both + bd_in[h, q].astype(F32)
            adds = [adds[s] + a_in[h, q, s].astype(F32) for s in range(subs)]
        spread = []
        for s in range(subs):
            turned = pltpu.roll(adds[s], rank, 1)
            spread.append(jnp.where(lower(turned), adds[s], turned))
            spread.append(jnp.where(lower(turned), turned, adds[s]))
        value = a_own[h] + extra[h] + jnp.concatenate(spread, axis=0)
        moved = pltpu.roll(both, rank, 1)
        value = value - jnp.where(lower(both), scale_0 * both, scale_0 * moved + scale_1 * both)
        owned[h] = value.reshape(groups, rows, lanes).astype(BF16)
        gossip_peers(lambda p: piece_copy(h, p, g).start())
        first[h, g] = owned[h, g]

    slab = min(16, step)

    def half_step(i):
        at = pl.ds(pl.multiple_of(i * slab, slab), slab)
        half_ref[0, at] = half_ref[0, at] - scale_0[0, 0] * gv[0, at].astype(F32) - scale_1[0, 0] * gv[1, at].astype(F32)

    each(0, gv.shape[1] // slab, half_step)

    gossip_peers(lambda p: pair_copy(p, p).wait())
    inside = lax.broadcasted_iota(jnp.int32, (rows, flat), 0).astype(F32)
    column = lax.broadcasted_iota(jnp.int32, (rows, flat), 1).astype(F32)
    for index in range(ROUNDS):
        blocks = []
        for replica in range(groups):
            wanted = pairs[replica, index : index + 1, 0:1] * float(rows) + inside
            blocks.append(jnp.where(wanted == column, 1.0, 0.0))
        choose[index] = jnp.concatenate(blocks, axis=0).astype(BF16)

    zeros = jnp.zeros((rank, lanes), F32)
    gram_high, gram_low = high_low(jnp.concatenate([gram, zeros], axis=0))
    unit_row = lax.broadcasted_iota(jnp.int32, (lanes, lanes), 0)
    unit_lane = lax.broadcasted_iota(jnp.int32, (lanes, lanes), 1)
    unit = jnp.where(unit_row % rank == unit_lane % rank, 1.0, 0.0).astype(BF16)

    def through(value):
        high, low = high_low(value)
        return dot(high, gram_high) + dot(low, gram_high) + dot(high, gram_low)

    for h in range(phases):
        gossip_peers(lambda p: piece_copy(h, p, p).wait())
        state = first[h].astype(F32).reshape(flat, lanes)
        narrow = state.astype(BF16)
        apart = dot(choose[0], narrow) - state
        again = (dot(narrow, unit) + through(mixing * apart - state)).astype(BF16)
        sent = again.astype(F32)
        later = dot(choose[1], again) - sent
        answer = jnp.where(lower(sent), mixing * (apart + later), sent)
        reply[h] = answer.reshape(groups, rows, lanes).astype(BF16)
        each(1, count, lambda k: result_copy(h, k, me, g, m).start())
        final[h, m, g] = reply[h, g]
        apart_ref[0, h] = jnp.where(lower(apart), apart, 0.0)
        apart_ref[1, h] = jnp.where(lower(later), later, 0.0)

    for index in range(ROUNDS):
        moved = jnp.zeros((), F32)
        for h in range(phases):
            value = apart_ref[index, h]
            moved = moved + jnp.sum(value * through(value))
        cons[me, index : index + 1] = jnp.full((1, lanes), moved, F32)
    wide_start(1, cons)
    for h in range(phases):
        def result_finish(k):
            d, p, q = device(k)
            result_copy(h, k, d, p, q).wait()
        each(1, count, result_finish)
    f_ref[...] = final[...].astype(F32).reshape(f_ref.shape)
    wide_finish(1, cons)
    stat_ref[0] = norm
    stat_ref[1] = jnp.sum(cons[...], axis=0) / total


def blend(h_ref, f_ref, b_ref, stat_ref, out_hbm, c_hbm, drift_hbm, norm_hbm,
          tiles, coefs, drift, norm, stores, others):
    rank, height = coefs.shape
    steps = stores.shape[0]
    step = height // steps

    def store(i):
        at = pl.ds(pl.multiple_of(i * step, step), step)
        return pltpu.make_async_copy(tiles.at[at], out_hbm.at[0, at], stores.at[i])

    def work(i):
        at = pl.ds(pl.multiple_of(i * step, step), step)
        part = f_ref[at, :rank].astype(BF16)
        tiles[at] = h_ref[0, at] + dot(jnp.concatenate([part, part], axis=1), b_ref[...])
        store(i).start()

    each(0, steps, work)
    for index in range(ROUNDS):
        norm[index] = jnp.max(stat_ref[0, index : index + 1, :])
        drift[index] = jnp.max(stat_ref[1, index : index + 1, :])
    coefs[...] = f_ref[...].T[rank:]
    copies = [pltpu.make_async_copy(coefs, c_hbm, others.at[0]), pltpu.make_async_copy(drift, drift_hbm, others.at[1]),
              pltpu.make_async_copy(norm, norm_hbm, others.at[2])]
    for copy in copies:
        copy.start()
    for copy in copies:
        copy.wait()
    each(0, steps, lambda i: store(i).wait())


def body(params, public, gradients, projection, partners):
    groups = lax.axis_size("gossip")
    members = lax.axis_size("mp")
    _, height, columns = params.shape
    rank = projection.shape[1]
    lanes = 2 * rank
    count = groups * members
    total = height * columns * count
    phases = 2 if height % (32 * count) == 0 else 1
    rows = height // (count * phases)
    block = height // (members * phases)
    step = min(128, block)
    subs = block // step
    steps = height // step
    flat = groups * rows
    dma = pltpu.SemaphoreType.DMA
    half, final, basis, stats = pl.pallas_call(
        functools.partial(exchange, groups, members, total),
        in_specs=[HBM] * 5,
        out_specs=[VMEM, VMEM, VMEM, VMEM],
        out_shape=[pltpu.VMEM(params.shape, F32), pltpu.VMEM((height, lanes), F32),
                   pltpu.VMEM((lanes, columns), BF16), pltpu.VMEM((2, ROUNDS, lanes), F32)],
        scratch_shapes=[
            pltpu.VMEM((ROUNDS, height, columns), BF16),
            pltpu.VMEM((rank, height), F32),
            pltpu.VMEM((rank, columns), F32),
            pltpu.SMEM((ROUNDS,), jnp.int32),
            pltpu.VMEM((ROUNDS, 8, columns), F32),
            pltpu.VMEM((phases, block, lanes), F32),
            pltpu.VMEM((phases, block, lanes), F32),
            pltpu.VMEM((phases, block, lanes), F32),
            pltpu.VMEM((phases, members, block, lanes), BF16),
            pltpu.VMEM((phases, members, block, lanes), BF16),
            pltpu.VMEM((phases, members, subs, step // 2, lanes), BF16),
            pltpu.VMEM((phases, members, subs, step // 2, lanes), BF16),
            pltpu.VMEM((members, rank, lanes), F32),
            pltpu.VMEM((count, ROUNDS, lanes), F32),
            pltpu.VMEM((groups, ROUNDS, lanes), F32),
            pltpu.VMEM((count, ROUNDS, lanes), F32),
            pltpu.VMEM((phases, groups, rows, lanes), BF16),
            pltpu.VMEM((phases, groups, rows, lanes), BF16),
            pltpu.VMEM((ROUNDS, flat, flat), BF16),
            pltpu.VMEM((ROUNDS, phases, flat, lanes), F32),
            pltpu.VMEM((phases, groups, rows, lanes), BF16),
            pltpu.VMEM((phases, members, groups, rows, lanes), BF16),
            dma((steps,)), dma((steps,)), dma((3,)),
            dma((2, count)), dma((2, count)), dma((phases + 1, groups)), dma((phases + 1, groups)),
            dma((members,)), dma((members,)), dma((2, phases, members)), dma((2, phases, members)),
            dma((phases, count)), dma((phases, count)),
        ],
        compiler_params=pltpu.CompilerParams(collective_id=0, has_side_effects=True, vmem_limit_bytes=30 << 20),
        name="exchange",
    )(*[pltpu.with_memory_space_constraint(value, pltpu.HBM) for value in
        (params, gradients, public[0].T, projection.T, partners.reshape(ROUNDS))])

    weights, coefs, drift, norm = pl.pallas_call(
        blend,
        in_specs=[VMEM, VMEM, VMEM, VMEM],
        out_specs=[ANYWHERE, ANYWHERE, ANYWHERE, ANYWHERE],
        out_shape=[jax.ShapeDtypeStruct(params.shape, F32), jax.ShapeDtypeStruct((rank, height), F32),
                   jax.ShapeDtypeStruct((ROUNDS,), F32), jax.ShapeDtypeStruct((ROUNDS,), F32)],
        scratch_shapes=[pltpu.VMEM((height, columns), F32), pltpu.VMEM((rank, height), F32),
                        pltpu.SMEM((ROUNDS,), F32), pltpu.SMEM((ROUNDS,), F32),
                        dma((height // min(128, height),)), dma((3,))],
        compiler_params=pltpu.CompilerParams(vmem_limit_bytes=20 << 20),
        name="blend",
    )(half, final, basis, stats)
    return (weights, coefs.T[None], drift, norm)


def solution(mesh):
    return jax.shard_map(
        body,
        mesh=mesh,
        in_specs=(
            P("gossip", None, "mp"),
            P("gossip", None, None),
            P(None, "gossip", None, "mp"),
            P("mp", None),
            P(None, "gossip"),
        ),
        out_specs=(P("gossip", None, "mp"), P("gossip", None, None), P(), P()),
        check_vma=False,
    )
```

```python
import functools

import jax
import jax.numpy as jnp
from jax import lax
from jax.experimental import pallas as pl
from jax.experimental.pallas import tpu as pltpu
from jax.sharding import PartitionSpec as P

ROUNDS = 2
step_size = 1.0
clip_limit = 0.5
mixing = 0.4
epsilon = 1e-06

F32 = jnp.float32
BF16 = jnp.bfloat16
VMEM = pl.BlockSpec(memory_space=pltpu.VMEM)
HBM = pl.BlockSpec(memory_space=pltpu.HBM)
ANYWHERE = pl.BlockSpec(memory_space=pl.ANY)
MESH = pl.DeviceIdType.MESH


def high_low(value):
    high = value.astype(BF16)
    return high, (value - high.astype(F32)).astype(BF16)


def dot(a, b):
    return jnp.dot(a, b, preferred_element_type=F32)


def dot_t(a, b):
    return lax.dot_general(a, b, (((1,), (1,)), ((), ())), preferred_element_type=F32)


def t_dot(a, b):
    return lax.dot_general(a, b, (((0,), (0,)), ((), ())), preferred_element_type=F32)


def each(low, high, act):
    lax.fori_loop(low, high, lambda i, _: (act(i), 0)[1], 0)


def exchange(groups, members, total, w_hbm, g_hbm, c_hbm, p_hbm, partners_hbm,
             half_ref, f_ref, basis, stat_ref,
             tall, gv, cv, pv, partners_ref, squares, kept, extra, leave, land, grams,
             norms, pairs, cons, owned, first, choose, apart_ref, reply, final,
             load_g, load_w, load_p, send, recv):
    g = lax.axis_index("gossip")
    m = lax.axis_index("mp")
    count = groups * members
    me = g * members + m
    phases, block, lanes = extra.shape
    subs = land.shape[3]
    step = block // subs
    steps = phases * members * subs
    rows = owned.shape[2]
    flat = groups * rows
    rank = lanes // 2
    columns = gv.shape[2]

    def wrap(value, size):
        return jnp.where(value >= size, value - size, value)

    def place(j):
        return j % phases, wrap(m + j // phases + 1, members)

    def span(i):
        h, q = place(i // subs)
        return pl.ds(pl.multiple_of((h * members + q) * block + (i % subs) * step, step), step)

    def grad_copy(i):
        return pltpu.make_async_copy(g_hbm.at[:, 0, span(i)], gv.at[:, span(i)], load_g.at[i])

    def weight_copy(i):
        return pltpu.make_async_copy(w_hbm.at[0, span(i)], half_ref.at[0, span(i)], load_w.at[i])

    basis_copy = pltpu.make_async_copy(p_hbm, pv, load_p.at[0])
    public_copy = pltpu.make_async_copy(c_hbm, cv, load_p.at[1])
    partners_copy = pltpu.make_async_copy(partners_hbm, partners_ref, load_p.at[2])
    basis_copy.start()
    partners_copy.start()
    each(0, steps, lambda i: grad_copy(i).start())

    def partner(k):
        return jnp.bitwise_xor(g, groups - k) if groups & (groups - 1) == 0 else wrap(g + k, groups)

    unroll = next(size for size in (5, 4, 3, 2, 1) if (groups - 1) % size == 0)

    def gossip_peers(act):
        each(0, (groups - 1) // unroll, lambda j: [act(partner(1 + j * unroll + k)) for k in range(unroll)])

    def mp_peers(act):
        for turn in range(1, members):
            act(wrap(m + turn, members))

    def all_peers(act):
        gossip_peers(lambda p: [act(p, wrap(m + turn, members)) for turn in range(members)])
        mp_peers(lambda q: act(g, q))

    barrier = pltpu.get_barrier_semaphore()

    def copy(slot, source, target, **device):
        return pltpu.make_async_remote_copy(src_ref=source, dst_ref=target, send_sem=send.at[slot],
                                            recv_sem=recv.at[slot], device_id=device, device_id_type=MESH)

    def finish(slot, ref):
        copy(slot, ref, ref, gossip=wrap(g + 1, groups), mp=m).wait()

    all_peers(lambda p, q: pl.semaphore_signal(barrier, inc=1, device_id={"gossip": p, "mp": q}, device_id_type=MESH))

    NORM, CONS, PAIR, GRAM = range(4)
    FIRST, SECOND, WEIGHT, PIECE, RESULT = range(5)

    def slot(kind, h):
        return 4 + kind * phases + h

    squares[...] = jnp.zeros_like(squares)
    basis_copy.wait()
    high, low = high_low(pv[...])
    basis[...] = jnp.concatenate([high, low], axis=0)
    tall[...] = jnp.concatenate([high.astype(F32), low.astype(F32)], axis=0).T.astype(BF16)

    def fold(value):
        return value + pltpu.roll(value, rank, 1)

    def lower(value):
        return lax.broadcasted_iota(jnp.int32, value.shape, value.ndim - 1) < rank

    def pack(value):
        half = value.shape[0] // 2
        return jnp.where(lower(value[:half]), value[:half], value[half:]).astype(BF16)

    lead = steps // 2
    others = phases * (members - 1)

    def square_step(i):
        grad_copy(i).wait()

        @pl.when(i >= lead)
        def _():
            weight_copy(i - lead).start()

        for index in range(ROUNDS):
            wide = gv[index, span(i)].astype(F32)
            squares[index] += jnp.sum((wide * wide).reshape(step // 8, 8, columns), axis=0)

    def send_step(i):
        square_step(i)
        h, q = place(i // subs)
        leave[FIRST, h, q, i % subs] = pack(fold(dot(gv[0, span(i)], tall[...])))

    def keep_step(i):
        square_step(i)
        h, _ = place(i // subs)
        kept[FIRST, h, pl.ds(pl.multiple_of((i % subs) * step, step), step)] = dot(gv[0, span(i)], tall[...])

    each(0, others * subs, send_step)
    early = max(others * subs, steps * 5 // 8)
    each(others * subs, early, keep_step)
    pl.semaphore_wait(barrier, count - 1)
    for h in range(phases):
        mp_peers(lambda q: copy(slot(FIRST, h), leave.at[FIRST, h, q], land.at[FIRST, h, m], mp=q).start())
    each(early, steps, keep_step)
    each(steps - lead, steps, lambda i: weight_copy(i).start())
    public_copy.start()
    partners_copy.wait()
    for index in range(ROUNDS):
        norms[me, index : index + 1] = jnp.full((1, lanes), jnp.sum(squares[index]), F32)
        pairs[g, index : index + 1] = jnp.full((1, lanes), partners_ref[index].astype(F32), F32)

    all_peers(lambda p, q: copy(NORM, norms.at[me], norms.at[me], gossip=p, mp=q).start())

    parts = dot_t(basis[...], basis[...])
    folded = parts + pltpu.roll(parts, rank, 1)
    grams[m] = folded[:rank] + folded[rank:]
    mp_peers(lambda q: copy(GRAM, grams.at[m], grams.at[m], mp=q).start())

    def rows_of(j):
        h, q = place(j)
        return pl.ds(pl.multiple_of((h * members + q) * block, block), block)

    def value_of(kind, j):
        if kind == WEIGHT:
            each(j * subs, (j + 1) * subs, lambda i: weight_copy(i).wait())
            return half_ref[0, rows_of(j)].astype(BF16)
        return gv[kind, rows_of(j)]

    def multiply(kind, j):
        product = dot(value_of(kind, j), tall[...])
        h, q = j % phases, wrap(m + j // phases + 1, members)
        if j >= others:
            kept[kind, h] = product
        else:
            product = fold(product)
            leave[kind, h, q] = jnp.stack([pack(product[at : at + step]) for at in range(0, block, step)])
            copy(slot(kind, h), leave.at[kind, h, q], land.at[kind, h, m], mp=q).start()

    for low, high in ((0, others), (others, phases * members)):
        for j in range(low, high):
            with jax.named_scope('second'):
                multiply(SECOND, j)
        for j in range(low, high):
            with jax.named_scope('weight'):
                multiply(WEIGHT, j)
        if low == 0:
            gossip_peers(lambda p: copy(PAIR, pairs.at[g], pairs.at[g], gossip=p).start())

    finish(GRAM, grams.at[pl.ds(0, members - 1)])
    gram = grams[0]
    for index in range(1, members):
        gram = gram + grams[index]
    gram_row = lax.broadcasted_iota(jnp.int32, gram.shape, 0)
    gram_lane = lax.broadcasted_iota(jnp.int32, gram.shape, 1)
    mixer_high, mixer_low = high_low(jnp.where(gram_lane < rank, jnp.where(gram_row == gram_lane, 1.0, 0.0) - gram, 0.0))
    public_copy.wait()
    for h in range(phases):
        at = pl.ds(pl.multiple_of((h * members + m) * block, block), block)
        high, low = high_low(cv[:, at])
        extra[h] = t_dot(high, mixer_high) + t_dot(low, mixer_high) + t_dot(high, mixer_low)

    finish(NORM, norms.at[pl.ds(0, count - 1)])
    norm = jnp.sqrt(jnp.sum(norms[...], axis=0) / total + epsilon)
    scale = step_size * jnp.minimum(1.0, clip_limit / norm)
    scale_0 = scale[0:1]
    scale_1 = scale[1:2]

    for h in range(phases):
        for kind in (FIRST, SECOND, WEIGHT):
            finish(slot(kind, h), land.at[kind, h, pl.ds(0, members - 1)])
        now = kept[WEIGHT, h] - scale_0 * kept[FIRST, h]
        value = jnp.where(lower(now), extra[h] + fold(now), fold(now - scale_1 * kept[SECOND, h]))
        for turn in range(1, members):
            q = wrap(m + turn, members)
            spread = []
            for sub in range(subs):
                first_, second_, weight_ = (land[kind, h, q, sub].astype(F32) for kind in (FIRST, SECOND, WEIGHT))
                now = weight_ - scale_0 * first_
                then = now - scale_1 * second_
                spread.append(jnp.where(lower(now), now, pltpu.roll(then, rank, 1)))
                spread.append(jnp.where(lower(now), pltpu.roll(now, rank, 1), then))
            value = value + jnp.concatenate(spread, axis=0)
        owned[h] = value.reshape(groups, rows, lanes).astype(BF16)
        gossip_peers(lambda p: copy(slot(PIECE, h), owned.at[h, p], first.at[h, g], gossip=p).start())
        first[h, g] = owned[h, g]

    slab = min(16, step)

    factor_0 = scale_0[0, 0]
    factor_1 = scale_1[0, 0]

    def half_step(i):
        at = pl.ds(pl.multiple_of(i * slab, slab), slab)
        half_ref[0, at] = half_ref[0, at] - factor_0 * gv[0, at].astype(F32) - factor_1 * gv[1, at].astype(F32)

    each(0, gv.shape[1] // slab, half_step)

    finish(PAIR, pairs.at[pl.ds(0, groups - 1)])
    inside = lax.broadcasted_iota(jnp.int32, (rows, flat), 0).astype(F32)
    column = lax.broadcasted_iota(jnp.int32, (rows, flat), 1).astype(F32)
    for index in range(ROUNDS):
        blocks = []
        for replica in range(groups):
            wanted = pairs[replica, index : index + 1, 0:1] * float(rows) + inside
            blocks.append(jnp.where(wanted == column, 1.0, 0.0))
        choose[index] = jnp.concatenate(blocks, axis=0).astype(BF16)

    zeros = jnp.zeros((rank, lanes), F32)
    gram_high, gram_low = high_low(jnp.concatenate([gram, zeros], axis=0))
    unit_row = lax.broadcasted_iota(jnp.int32, (lanes, lanes), 0)
    unit_lane = lax.broadcasted_iota(jnp.int32, (lanes, lanes), 1)
    unit = jnp.where(unit_row % rank == unit_lane % rank, 1.0, 0.0).astype(BF16)

    def through(value):
        high, low = high_low(value)
        return dot(high, gram_high) + dot(low, gram_high) + dot(high, gram_low)

    for h in range(phases):
        finish(slot(PIECE, h), first.at[h, pl.ds(0, groups - 1)])
        state = first[h].astype(F32).reshape(flat, lanes)
        narrow = state.astype(BF16)
        apart = dot(choose[0], narrow) - state
        again = (dot(narrow, unit) + through(mixing * apart - state)).astype(BF16)
        sent = again.astype(F32)
        later = dot(choose[1], again) - sent
        answer = jnp.where(lower(sent), mixing * (apart + later), sent)
        reply[h] = answer.reshape(groups, rows, lanes).astype(BF16)
        all_peers(lambda p, q: copy(slot(RESULT, h), reply.at[h, p], final.at[h, m * groups + g], gossip=p, mp=q).start())
        final[h, m * groups + g] = reply[h, g]
        apart_ref[0, h] = jnp.where(lower(apart), apart, 0.0)
        apart_ref[1, h] = jnp.where(lower(later), later, 0.0)

    for index in range(ROUNDS):
        moved = jnp.zeros((), F32)
        for h in range(phases):
            value = apart_ref[index, h]
            moved = moved + jnp.sum(value * through(value))
        cons[me, index : index + 1] = jnp.full((1, lanes), moved, F32)
    all_peers(lambda p, q: copy(CONS, cons.at[me], cons.at[me], gossip=p, mp=q).start())
    for h in range(phases):
        finish(slot(RESULT, h), final.at[h, pl.ds(0, count - 1)])
    f_ref[...] = final[...].astype(F32).reshape(f_ref.shape)
    finish(CONS, cons.at[pl.ds(0, count - 1)])
    stat_ref[0] = norm
    stat_ref[1] = jnp.sum(cons[...], axis=0) / total


def blend(h_ref, f_ref, b_ref, stat_ref, out_hbm, c_hbm, drift_hbm, norm_hbm,
          tiles, coefs, drift, norm, stores, others):
    rank, height = coefs.shape
    steps = stores.shape[0]
    step = height // steps

    def store(i):
        at = pl.ds(pl.multiple_of(i * step, step), step)
        return pltpu.make_async_copy(tiles.at[at], out_hbm.at[0, at], stores.at[i])

    def work(i):
        at = pl.ds(pl.multiple_of(i * step, step), step)
        part = f_ref[at, :rank].astype(BF16)
        tiles[at] = h_ref[0, at] + dot(jnp.concatenate([part, part], axis=1), b_ref[...])
        store(i).start()

    each(0, steps, work)
    for index in range(ROUNDS):
        norm[index] = jnp.max(stat_ref[0, index : index + 1, :])
        drift[index] = jnp.max(stat_ref[1, index : index + 1, :])
    coefs[...] = f_ref[...].T[rank:]
    copies = [pltpu.make_async_copy(coefs, c_hbm, others.at[0]), pltpu.make_async_copy(drift, drift_hbm, others.at[1]),
              pltpu.make_async_copy(norm, norm_hbm, others.at[2])]
    for copy in copies:
        copy.start()
    for copy in copies:
        copy.wait()
    each(0, steps, lambda i: store(i).wait())


def body(params, public, gradients, projection, partners):
    groups = lax.axis_size("gossip")
    members = lax.axis_size("mp")
    _, height, columns = params.shape
    rank = projection.shape[1]
    lanes = 2 * rank
    count = groups * members
    total = height * columns * count
    phases = 2 if height % (32 * count) == 0 else 1
    rows = height // (count * phases)
    block = height // (members * phases)
    step = min(128, block)
    subs = block // step
    steps = height // step
    flat = groups * rows
    dma = pltpu.SemaphoreType.DMA
    half, final, basis, stats = pl.pallas_call(
        functools.partial(exchange, groups, members, total),
        in_specs=[HBM] * 5,
        out_specs=[VMEM, VMEM, VMEM, VMEM],
        out_shape=[pltpu.VMEM(params.shape, F32), pltpu.VMEM((height, lanes), F32),
                   pltpu.VMEM((lanes, columns), BF16), pltpu.VMEM((2, ROUNDS, lanes), F32)],
        scratch_shapes=[
            pltpu.VMEM((columns, lanes), BF16),
            pltpu.VMEM((ROUNDS, height, columns), BF16),
            pltpu.VMEM((rank, height), F32),
            pltpu.VMEM((rank, columns), F32),
            pltpu.SMEM((ROUNDS,), jnp.int32),
            pltpu.VMEM((ROUNDS, 8, columns), F32),
            pltpu.VMEM((3, phases, block, lanes), F32),
            pltpu.VMEM((phases, block, lanes), F32),
            pltpu.VMEM((3, phases, members, subs, step // 2, lanes), BF16),
            pltpu.VMEM((3, phases, members, subs, step // 2, lanes), BF16),
            pltpu.VMEM((members, rank, lanes), F32),
            pltpu.VMEM((count, ROUNDS, lanes), F32),
            pltpu.VMEM((groups, ROUNDS, lanes), F32),
            pltpu.VMEM((count, ROUNDS, lanes), F32),
            pltpu.VMEM((phases, groups, rows, lanes), BF16),
            pltpu.VMEM((phases, groups, rows, lanes), BF16),
            pltpu.VMEM((ROUNDS, flat, flat), BF16),
            pltpu.VMEM((ROUNDS, phases, flat, lanes), F32),
            pltpu.VMEM((phases, groups, rows, lanes), BF16),
            pltpu.VMEM((phases, count, rows, lanes), BF16),
            dma((steps,)), dma((steps,)), dma((3,)),
            dma((4 + 5 * phases,)), dma((4 + 5 * phases,)),
        ],
        compiler_params=pltpu.CompilerParams(collective_id=0, has_side_effects=True, vmem_limit_bytes=30 << 20),
        name="exchange",
    )(*[pltpu.with_memory_space_constraint(value, pltpu.HBM) for value in
        (params, gradients, public[0].T, projection.T, partners.reshape(ROUNDS))])

    weights, coefs, drift, norm = pl.pallas_call(
        blend,
        in_specs=[VMEM, VMEM, VMEM, VMEM],
        out_specs=[ANYWHERE, ANYWHERE, ANYWHERE, ANYWHERE],
        out_shape=[jax.ShapeDtypeStruct(params.shape, F32), jax.ShapeDtypeStruct((rank, height), F32),
                   jax.ShapeDtypeStruct((ROUNDS,), F32), jax.ShapeDtypeStruct((ROUNDS,), F32)],
        scratch_shapes=[pltpu.VMEM((height, columns), F32), pltpu.VMEM((rank, height), F32),
                        pltpu.SMEM((ROUNDS,), F32), pltpu.SMEM((ROUNDS,), F32),
                        dma((height // min(128, height),)), dma((3,))],
        compiler_params=pltpu.CompilerParams(vmem_limit_bytes=20 << 20),
        name="blend",
    )(half, final, basis, stats)
    return (weights, coefs.T[None], drift, norm)


def solution(mesh):
    return jax.shard_map(
        body,
        mesh=mesh,
        in_specs=(
            P("gossip", None, "mp"),
            P("gossip", None, None),
            P(None, "gossip", None, "mp"),
            P("mp", None),
            P(None, "gossip"),
        ),
        out_specs=(P("gossip", None, "mp"), P("gossip", None, None), P(), P()),
        check_vma=False,
    )
```

```python
import functools

import jax
import jax.numpy as jnp
from jax import lax
from jax.experimental import pallas as pl
from jax.experimental.pallas import tpu as pltpu
from jax.sharding import PartitionSpec as P

ROUNDS = 2
step_size = 1.0
clip_limit = 0.5
mixing = 0.4
epsilon = 1e-06

F32 = jnp.float32
BF16 = jnp.bfloat16
VMEM = pl.BlockSpec(memory_space=pltpu.VMEM)
HBM = pl.BlockSpec(memory_space=pltpu.HBM)
ANYWHERE = pl.BlockSpec(memory_space=pl.ANY)
MESH = pl.DeviceIdType.MESH


def high_low(value):
    high = value.astype(BF16)
    return high, (value - high.astype(F32)).astype(BF16)


def dot(a, b):
    return jnp.dot(a, b, preferred_element_type=F32)


def dot_t(a, b):
    return lax.dot_general(a, b, (((1,), (1,)), ((), ())), preferred_element_type=F32)


def t_dot(a, b):
    return lax.dot_general(a, b, (((0,), (0,)), ((), ())), preferred_element_type=F32)


def each(low, high, act):
    lax.fori_loop(low, high, lambda i, _: (act(i), 0)[1], 0)


def exchange(groups, members, total, w_hbm, g_hbm, c_hbm, p_hbm, partners_hbm,
             half_ref, f_ref, basis, stat_ref,
             tall, gv, cv, pv, partners_ref, squares, kept, extra, leave, land, grams,
             norms, pairs, cons, owned, first, choose, apart_ref, reply, final,
             load_g, load_w, load_p, send, recv):
    g = lax.axis_index("gossip")
    m = lax.axis_index("mp")
    count = groups * members
    me = g * members + m
    phases, block, lanes = extra.shape
    subs = land.shape[3]
    step = block // subs
    steps = phases * members * subs
    rows = owned.shape[2]
    flat = groups * rows
    rank = lanes // 2
    columns = gv.shape[2]

    def wrap(value, size):
        return jnp.where(value >= size, value - size, value)

    def place(j):
        return j % phases, wrap(m + j // phases + 1, members)

    def span(i):
        h, q = place(i // subs)
        return pl.ds(pl.multiple_of((h * members + q) * block + (i % subs) * step, step), step)

    def grad_copy(i):
        return pltpu.make_async_copy(g_hbm.at[:, 0, span(i)], gv.at[:, span(i)], load_g.at[i])

    def weight_copy(i):
        return pltpu.make_async_copy(w_hbm.at[0, span(i)], half_ref.at[0, span(i)], load_w.at[i])

    basis_copy = pltpu.make_async_copy(p_hbm, pv, load_p.at[0])
    public_copy = pltpu.make_async_copy(c_hbm, cv, load_p.at[1])
    partners_copy = pltpu.make_async_copy(partners_hbm, partners_ref, load_p.at[2])
    basis_copy.start()
    partners_copy.start()
    each(0, steps, lambda i: grad_copy(i).start())

    def partner(k):
        return jnp.bitwise_xor(g, groups - k) if groups & (groups - 1) == 0 else wrap(g + k, groups)

    def some_peers(low, high, act):
        unroll = next(size for size in (5, 4, 3, 2, 1) if (high - low) % size == 0)
        each(0, (high - low) // unroll, lambda j: [act(partner(low + j * unroll + k)) for k in range(unroll)])

    def gossip_peers(act):
        some_peers(1, groups, act)

    def mp_peers(act):
        for turn in range(1, members):
            act(wrap(m + turn, members))

    def all_peers(act):
        gossip_peers(lambda p: [act(p, wrap(m + turn, members)) for turn in range(members)])
        mp_peers(lambda q: act(g, q))

    barrier = pltpu.get_barrier_semaphore()

    def copy(slot, source, target, **device):
        return pltpu.make_async_remote_copy(src_ref=source, dst_ref=target, send_sem=send.at[slot],
                                            recv_sem=recv.at[slot], device_id=device, device_id_type=MESH)

    def finish(slot, ref):
        copy(slot, ref, ref, gossip=wrap(g + 1, groups), mp=m).wait()

    all_peers(lambda p, q: pl.semaphore_signal(barrier, inc=1, device_id={"gossip": p, "mp": q}, device_id_type=MESH))

    NORM, CONS, PAIR, GRAM = range(4)
    FIRST, SECOND, WEIGHT, PIECE, RESULT, FAR, RELAY = range(7)

    def slot(kind, h):
        return 4 + kind * phases + h

    squares[...] = jnp.zeros_like(squares)
    basis_copy.wait()
    high, low = high_low(pv[...])
    basis[...] = jnp.concatenate([high, low], axis=0)
    tall[...] = jnp.concatenate([high.astype(F32), low.astype(F32)], axis=0).T.astype(BF16)

    def fold(value):
        return value + pltpu.roll(value, rank, 1)

    def lower(value):
        return lax.broadcasted_iota(jnp.int32, value.shape, value.ndim - 1) < rank

    def pack(value):
        half = value.shape[0] // 2
        return jnp.where(lower(value[:half]), value[:half], value[half:]).astype(BF16)

    lead = steps // 2
    others = phases * (members - 1)
    relayed = phases // 2 if groups & (groups - 1) == 0 and members > 1 else 0

    def square_step(i):
        grad_copy(i).wait()

        @pl.when(i >= lead)
        def _():
            weight_copy(i - lead).start()

        for index in range(ROUNDS):
            wide = gv[index, span(i)].astype(F32)
            squares[index] += jnp.sum((wide * wide).reshape(step // 8, 8, columns), axis=0)

    def send_step(i):
        square_step(i)
        h, q = place(i // subs)
        leave[FIRST, h, q, i % subs] = pack(fold(dot(gv[0, span(i)], tall[...])))

    def keep_step(i):
        square_step(i)
        h, _ = place(i // subs)
        kept[FIRST, h, pl.ds(pl.multiple_of((i % subs) * step, step), step)] = dot(gv[0, span(i)], tall[...])

    each(0, others * subs, send_step)
    early = max(others * subs, steps * 5 // 8)
    each(others * subs, early, keep_step)
    pl.semaphore_wait(barrier, count - 1)
    for h in range(phases):
        mp_peers(lambda q: copy(slot(FIRST, h), leave.at[FIRST, h, q], land.at[FIRST, h, m], mp=q).start())
    each(early, steps, keep_step)
    each(steps - lead, steps, lambda i: weight_copy(i).start())
    public_copy.start()
    partners_copy.wait()
    for index in range(ROUNDS):
        norms[me, index : index + 1] = jnp.full((1, lanes), jnp.sum(squares[index]), F32)
        pairs[g, index : index + 1] = jnp.full((1, lanes), partners_ref[index].astype(F32), F32)

    all_peers(lambda p, q: copy(NORM, norms.at[me], norms.at[me], gossip=p, mp=q).start())

    parts = dot_t(basis[...], basis[...])
    folded = parts + pltpu.roll(parts, rank, 1)
    grams[m] = folded[:rank] + folded[rank:]
    mp_peers(lambda q: copy(GRAM, grams.at[m], grams.at[m], mp=q).start())

    def rows_of(j):
        h, q = place(j)
        return pl.ds(pl.multiple_of((h * members + q) * block, block), block)

    def value_of(kind, j):
        if kind == WEIGHT:
            each(j * subs, (j + 1) * subs, lambda i: weight_copy(i).wait())
            return half_ref[0, rows_of(j)].astype(BF16)
        return gv[kind, rows_of(j)]

    def multiply(kind, j):
        product = dot(value_of(kind, j), tall[...])
        h, q = j % phases, wrap(m + j // phases + 1, members)
        if j >= others:
            kept[kind, h] = product
        else:
            product = fold(product)
            leave[kind, h, q] = jnp.stack([pack(product[at : at + step]) for at in range(0, block, step)])
            copy(slot(kind, h), leave.at[kind, h, q], land.at[kind, h, m], mp=q).start()

    for low, high in ((0, others), (others, phases * members)):
        for j in range(low, high):
            with jax.named_scope('second'):
                multiply(SECOND, j)
        for j in range(low, high):
            with jax.named_scope('weight'):
                multiply(WEIGHT, j)
        if low == 0:
            gossip_peers(lambda p: copy(PAIR, pairs.at[g], pairs.at[g], gossip=p).start())

    finish(GRAM, grams.at[pl.ds(0, members - 1)])
    gram = grams[0]
    for index in range(1, members):
        gram = gram + grams[index]
    gram_row = lax.broadcasted_iota(jnp.int32, gram.shape, 0)
    gram_lane = lax.broadcasted_iota(jnp.int32, gram.shape, 1)
    mixer_high, mixer_low = high_low(jnp.where(gram_lane < rank, jnp.where(gram_row == gram_lane, 1.0, 0.0) - gram, 0.0))
    public_copy.wait()
    for h in range(phases):
        at = pl.ds(pl.multiple_of((h * members + m) * block, block), block)
        high, low = high_low(cv[:, at])
        extra[h] = t_dot(high, mixer_high) + t_dot(low, mixer_high) + t_dot(high, mixer_low)

    finish(NORM, norms.at[pl.ds(0, count - 1)])
    norm = jnp.sqrt(jnp.sum(norms[...], axis=0) / total + epsilon)
    scale = step_size * jnp.minimum(1.0, clip_limit / norm)
    scale_0 = scale[0:1]
    scale_1 = scale[1:2]

    for h in range(phases):
        for kind in (FIRST, SECOND, WEIGHT):
            finish(slot(kind, h), land.at[kind, h, pl.ds(0, members - 1)])
        now = kept[WEIGHT, h] - scale_0 * kept[FIRST, h]
        value = jnp.where(lower(now), extra[h] + fold(now), fold(now - scale_1 * kept[SECOND, h]))
        for turn in range(1, members):
            q = wrap(m + turn, members)
            spread = []
            for sub in range(subs):
                first_, second_, weight_ = (land[kind, h, q, sub].astype(F32) for kind in (FIRST, SECOND, WEIGHT))
                now = weight_ - scale_0 * first_
                then = now - scale_1 * second_
                spread.append(jnp.where(lower(now), now, pltpu.roll(then, rank, 1)))
                spread.append(jnp.where(lower(now), pltpu.roll(now, rank, 1), then))
            value = value + jnp.concatenate(spread, axis=0)
        owned[h] = value.reshape(groups, rows, lanes).astype(BF16)
        gossip_peers(lambda p: copy(slot(PIECE, h), owned.at[h, p], first.at[h, g], gossip=p).start())
        first[h, g] = owned[h, g]

    slab = min(16, step)

    factor_0 = scale_0[0, 0]
    factor_1 = scale_1[0, 0]

    def half_step(i):
        at = pl.ds(pl.multiple_of(i * slab, slab), slab)
        half_ref[0, at] = half_ref[0, at] - factor_0 * gv[0, at].astype(F32) - factor_1 * gv[1, at].astype(F32)

    each(0, gv.shape[1] // slab, half_step)

    finish(PAIR, pairs.at[pl.ds(0, groups - 1)])
    inside = lax.broadcasted_iota(jnp.int32, (rows, flat), 0).astype(F32)
    column = lax.broadcasted_iota(jnp.int32, (rows, flat), 1).astype(F32)
    for index in range(ROUNDS):
        blocks = []
        for replica in range(groups):
            wanted = pairs[replica, index : index + 1, 0:1] * float(rows) + inside
            blocks.append(jnp.where(wanted == column, 1.0, 0.0))
        choose[index] = jnp.concatenate(blocks, axis=0).astype(BF16)

    zeros = jnp.zeros((rank, lanes), F32)
    gram_high, gram_low = high_low(jnp.concatenate([gram, zeros], axis=0))
    unit_row = lax.broadcasted_iota(jnp.int32, (lanes, lanes), 0)
    unit_lane = lax.broadcasted_iota(jnp.int32, (lanes, lanes), 1)
    unit = jnp.where(unit_row % rank == unit_lane % rank, 1.0, 0.0).astype(BF16)

    def through(value):
        high, low = high_low(value)
        return dot(high, gram_high) + dot(low, gram_high) + dot(high, gram_low)

    for h in range(phases):
        finish(slot(PIECE, h), first.at[h, pl.ds(0, groups - 1)])
    every = range(phases)
    state = [first[h].astype(F32).reshape(flat, lanes) for h in every]
    narrow = [state[h].astype(BF16) for h in every]
    apart = [dot(choose[0], narrow[h]) - state[h] for h in every]
    again = [(dot(narrow[h], unit) + through(mixing * apart[h] - state[h])).astype(BF16) for h in every]
    sent = [again[h].astype(F32) for h in every]
    later = [dot(choose[1], again[h]) - sent[h] for h in every]
    for h in every:
        answer = jnp.where(lower(sent[h]), mixing * (apart[h] + later[h]), sent[h])
        reply[h] = answer.reshape(groups, rows, lanes).astype(BF16)
    middle = groups // 2
    for h in every:
        def to_all(p):
            for turn in range(members):
                copy(slot(RESULT, h), reply.at[h, p], final.at[h, m * groups + g], gossip=p, mp=wrap(m + turn, members)).start()

        if h < relayed:
            some_peers(1, middle + 1, lambda p: copy(
                slot(FAR, h), reply.at[h, p], final.at[h, m * groups + g], gossip=p).start())
            some_peers(middle + 1, groups, to_all)
        else:
            gossip_peers(to_all)
        mp_peers(lambda q: copy(slot(RESULT, h), reply.at[h, g], final.at[h, m * groups + g], mp=q).start())
        final[h, m * groups + g] = reply[h, g]
    for h in every:
        apart_ref[0, h] = jnp.where(lower(apart[h]), apart[h], 0.0)
        apart_ref[1, h] = jnp.where(lower(later[h]), later[h], 0.0)

    for index in range(ROUNDS):
        moved = jnp.zeros((), F32)
        for h in range(phases):
            value = apart_ref[index, h]
            moved = moved + jnp.sum(value * through(value))
        cons[me, index : index + 1] = jnp.full((1, lanes), moved, F32)
    all_peers(lambda p, q: copy(CONS, cons.at[me], cons.at[me], gossip=p, mp=q).start())
    across = pl.ds(pl.multiple_of(m * groups + jnp.where(g >= middle, 0, middle), middle), middle)
    for h in range(relayed):
        finish(slot(FAR, h), final.at[h, pl.ds(0, middle)])
        mp_peers(lambda q: copy(slot(RELAY, h), final.at[h, across], final.at[h, across], mp=q).start())
    for h in every:
        if h < relayed:
            finish(slot(RELAY, h), final.at[h, pl.ds(0, (members - 1) * middle)])
            finish(slot(RESULT, h), final.at[h, pl.ds(0, members * middle - 1)])
        else:
            finish(slot(RESULT, h), final.at[h, pl.ds(0, count - 1)])
    f_ref[...] = final[...].astype(F32).reshape(f_ref.shape)
    finish(CONS, cons.at[pl.ds(0, count - 1)])
    stat_ref[0] = norm
    stat_ref[1] = jnp.sum(cons[...], axis=0) / total


def blend(h_ref, f_ref, b_ref, stat_ref, out_hbm, c_hbm, drift_hbm, norm_hbm,
          tiles, coefs, drift, norm, stores, others):
    rank, height = coefs.shape
    steps = stores.shape[0]
    step = height // steps

    def store(i):
        at = pl.ds(pl.multiple_of(i * step, step), step)
        return pltpu.make_async_copy(tiles.at[at], out_hbm.at[0, at], stores.at[i])

    def work(i):
        at = pl.ds(pl.multiple_of(i * step, step), step)
        part = f_ref[at, :rank].astype(BF16)
        tiles[at] = h_ref[0, at] + dot(jnp.concatenate([part, part], axis=1), b_ref[...])
        store(i).start()

    each(0, steps, work)
    for index in range(ROUNDS):
        norm[index] = jnp.max(stat_ref[0, index : index + 1, :])
        drift[index] = jnp.max(stat_ref[1, index : index + 1, :])
    coefs[...] = f_ref[...].T[rank:]
    copies = [pltpu.make_async_copy(coefs, c_hbm, others.at[0]), pltpu.make_async_copy(drift, drift_hbm, others.at[1]),
              pltpu.make_async_copy(norm, norm_hbm, others.at[2])]
    for copy in copies:
        copy.start()
    for copy in copies:
        copy.wait()
    each(0, steps, lambda i: store(i).wait())


def body(params, public, gradients, projection, partners):
    groups = lax.axis_size("gossip")
    members = lax.axis_size("mp")
    _, height, columns = params.shape
    rank = projection.shape[1]
    lanes = 2 * rank
    count = groups * members
    total = height * columns * count
    phases = 2 if height % (32 * count) == 0 else 1
    rows = height // (count * phases)
    block = height // (members * phases)
    step = min(128, block)
    subs = block // step
    steps = height // step
    flat = groups * rows
    dma = pltpu.SemaphoreType.DMA
    half, final, basis, stats = pl.pallas_call(
        functools.partial(exchange, groups, members, total),
        in_specs=[HBM] * 5,
        out_specs=[VMEM, VMEM, VMEM, VMEM],
        out_shape=[pltpu.VMEM(params.shape, F32), pltpu.VMEM((height, lanes), F32),
                   pltpu.VMEM((lanes, columns), BF16), pltpu.VMEM((2, ROUNDS, lanes), F32)],
        scratch_shapes=[
            pltpu.VMEM((columns, lanes), BF16),
            pltpu.VMEM((ROUNDS, height, columns), BF16),
            pltpu.VMEM((rank, height), F32),
            pltpu.VMEM((rank, columns), F32),
            pltpu.SMEM((ROUNDS,), jnp.int32),
            pltpu.VMEM((ROUNDS, 8, columns), F32),
            pltpu.VMEM((3, phases, block, lanes), F32),
            pltpu.VMEM((phases, block, lanes), F32),
            pltpu.VMEM((3, phases, members, subs, step // 2, lanes), BF16),
            pltpu.VMEM((3, phases, members, subs, step // 2, lanes), BF16),
            pltpu.VMEM((members, rank, lanes), F32),
            pltpu.VMEM((count, ROUNDS, lanes), F32),
            pltpu.VMEM((groups, ROUNDS, lanes), F32),
            pltpu.VMEM((count, ROUNDS, lanes), F32),
            pltpu.VMEM((phases, groups, rows, lanes), BF16),
            pltpu.VMEM((phases, groups, rows, lanes), BF16),
            pltpu.VMEM((ROUNDS, flat, flat), BF16),
            pltpu.VMEM((ROUNDS, phases, flat, lanes), F32),
            pltpu.VMEM((phases, groups, rows, lanes), BF16),
            pltpu.VMEM((phases, count, rows, lanes), BF16),
            dma((steps,)), dma((steps,)), dma((3,)),
            dma((4 + 7 * phases,)), dma((4 + 7 * phases,)),
        ],
        compiler_params=pltpu.CompilerParams(collective_id=0, has_side_effects=True, vmem_limit_bytes=30 << 20),
        name="exchange",
    )(*[pltpu.with_memory_space_constraint(value, pltpu.HBM) for value in
        (params, gradients, public[0].T, projection.T, partners.reshape(ROUNDS))])

    weights, coefs, drift, norm = pl.pallas_call(
        blend,
        in_specs=[VMEM, VMEM, VMEM, VMEM],
        out_specs=[ANYWHERE, ANYWHERE, ANYWHERE, ANYWHERE],
        out_shape=[jax.ShapeDtypeStruct(params.shape, F32), jax.ShapeDtypeStruct((rank, height), F32),
                   jax.ShapeDtypeStruct((ROUNDS,), F32), jax.ShapeDtypeStruct((ROUNDS,), F32)],
        scratch_shapes=[pltpu.VMEM((height, columns), F32), pltpu.VMEM((rank, height), F32),
                        pltpu.SMEM((ROUNDS,), F32), pltpu.SMEM((ROUNDS,), F32),
                        dma((height // min(128, height),)), dma((3,))],
        compiler_params=pltpu.CompilerParams(vmem_limit_bytes=20 << 20),
        name="blend",
    )(half, final, basis, stats)
    return (weights, coefs.T[None], drift, norm)


def solution(mesh):
    return jax.shard_map(
        body,
        mesh=mesh,
        in_specs=(
            P("gossip", None, "mp"),
            P("gossip", None, None),
            P(None, "gossip", None, "mp"),
            P("mp", None),
            P(None, "gossip"),
        ),
        out_specs=(P("gossip", None, "mp"), P("gossip", None, None), P(), P()),
        check_vma=False,
    )
```

```python
import functools

import jax
import jax.numpy as jnp
from jax import lax
from jax.experimental import pallas as pl
from jax.experimental.pallas import tpu as pltpu
from jax.sharding import PartitionSpec as P

ROUNDS = 2
step_size = 1.0
clip_limit = 0.5
mixing = 0.4
epsilon = 1e-06

F32 = jnp.float32
BF16 = jnp.bfloat16
VMEM = pl.BlockSpec(memory_space=pltpu.VMEM)
HBM = pl.BlockSpec(memory_space=pltpu.HBM)
ANYWHERE = pl.BlockSpec(memory_space=pl.ANY)
MESH = pl.DeviceIdType.MESH


def high_low(value):
    high = value.astype(BF16)
    return high, (value - high.astype(F32)).astype(BF16)


def dot(a, b):
    return jnp.dot(a, b, preferred_element_type=F32)


def dot_t(a, b):
    return lax.dot_general(a, b, (((1,), (1,)), ((), ())), preferred_element_type=F32)


def t_dot(a, b):
    return lax.dot_general(a, b, (((0,), (0,)), ((), ())), preferred_element_type=F32)


def each(low, high, act):
    lax.fori_loop(low, high, lambda i, _: (act(i), 0)[1], 0)


def exchange(groups, members, total, w_hbm, g_hbm, c_hbm, p_hbm, partners_hbm,
             half_ref, f_ref, basis, stat_ref,
             tall, gv, cv, pv, partners_ref, squares, kept, extra, leave, land, grams,
             norms, pairs, cons, owned, first, choose, apart_ref, reply, final,
             load_g, load_w, load_p, send, recv):
    g = lax.axis_index("gossip")
    m = lax.axis_index("mp")
    count = groups * members
    me = g * members + m
    phases, block, lanes = extra.shape
    subs = land.shape[3]
    step = block // subs
    steps = phases * members * subs
    rows = owned.shape[2]
    flat = groups * rows
    rank = lanes // 2
    columns = gv.shape[2]

    def wrap(value, size):
        return jnp.where(value >= size, value - size, value)

    def place(j):
        return j % phases, wrap(m + j // phases + 1, members)

    def span(i):
        h, q = place(i // subs)
        return pl.ds(pl.multiple_of((h * members + q) * block + (i % subs) * step, step), step)

    def grad_copy(i):
        return pltpu.make_async_copy(g_hbm.at[:, 0, span(i)], gv.at[:, span(i)], load_g.at[i])

    def rows_of(j):
        h, q = place(j)
        return pl.ds(pl.multiple_of((h * members + q) * block, block), block)

    def weight_copy(j):
        return pltpu.make_async_copy(w_hbm.at[0, rows_of(j)], half_ref.at[0, rows_of(j)], load_w.at[j])

    basis_copy = pltpu.make_async_copy(p_hbm, pv, load_p.at[0])
    public_copy = pltpu.make_async_copy(c_hbm, cv, load_p.at[1])
    partners_copy = pltpu.make_async_copy(partners_hbm, partners_ref, load_p.at[2])
    basis_copy.start()
    partners_copy.start()
    each(0, steps, lambda i: grad_copy(i).start())

    def partner(k):
        return jnp.bitwise_xor(g, groups - k) if groups & (groups - 1) == 0 else wrap(g + k, groups)

    def some_peers(low, high, act):
        unroll = next(size for size in (5, 4, 3, 2, 1) if (high - low) % size == 0)
        each(0, (high - low) // unroll, lambda j: [act(partner(low + j * unroll + k)) for k in range(unroll)])

    def gossip_peers(act):
        some_peers(1, groups, act)

    def mp_peers(act):
        for turn in range(1, members):
            act(wrap(m + turn, members))

    def all_peers(act):
        gossip_peers(lambda p: [act(p, wrap(m + turn, members)) for turn in range(members)])
        mp_peers(lambda q: act(g, q))

    barrier = pltpu.get_barrier_semaphore()

    def copy(slot, source, target, **device):
        return pltpu.make_async_remote_copy(src_ref=source, dst_ref=target, send_sem=send.at[slot],
                                            recv_sem=recv.at[slot], device_id=device, device_id_type=MESH)

    def finish(slot, ref):
        copy(slot, ref, ref, gossip=wrap(g + 1, groups), mp=m).wait()

    all_peers(lambda p, q: pl.semaphore_signal(barrier, inc=1, device_id={"gossip": p, "mp": q}, device_id_type=MESH))

    NORM, CONS, PAIR, GRAM = range(4)
    FIRST, SECOND, WEIGHT, PIECE, RESULT, FAR, RELAY = range(7)

    def slot(kind, h):
        return 4 + kind * phases + h

    squares[...] = jnp.zeros_like(squares)
    basis_copy.wait()
    high, low = high_low(pv[...])
    basis[...] = jnp.concatenate([high, low], axis=0)
    tall[...] = jnp.concatenate([high.astype(F32), low.astype(F32)], axis=0).T.astype(BF16)

    def fold(value):
        return value + pltpu.roll(value, rank, 1)

    def lower(value):
        return lax.broadcasted_iota(jnp.int32, value.shape, value.ndim - 1) < rank

    def pack(value):
        half = value.shape[0] // 2
        top, bottom = value[:half], value[half:]
        return (jnp.where(lower(top), top, bottom) + pltpu.roll(jnp.where(lower(top), bottom, top), rank, 1)).astype(BF16)

    blocks = phases * members
    lead = blocks // 2 * subs
    others = phases * (members - 1)
    relayed = phases // 2 if groups & (groups - 1) == 0 and members > 1 else 0

    def square_step(i):
        grad_copy(i).wait()

        @pl.when((i >= lead) & (i % subs == 0))
        def _():
            weight_copy((i - lead) // subs).start()

        for index in range(ROUNDS):
            wide = gv[index, span(i)].astype(F32)
            squares[index] += jnp.sum((wide * wide).reshape(step // 8, 8, columns), axis=0)

    def send_step(i):
        square_step(i)
        h, q = place(i // subs)
        leave[FIRST, h, q, i % subs] = pack(dot(gv[0, span(i)], tall[...]))

    def keep_step(i):
        square_step(i)
        h, _ = place(i // subs)
        kept[FIRST, h, pl.ds(pl.multiple_of((i % subs) * step, step), step)] = dot(gv[0, span(i)], tall[...])

    each(0, others * subs, send_step)
    early = max(others * subs, steps * 5 // 8)
    each(others * subs, early, keep_step)
    parts = dot_t(basis[...], basis[...])
    folded = parts + pltpu.roll(parts, rank, 1)
    full = folded[:rank] + folded[rank:]
    grams[m] = jnp.where(lower(full[: rank // 2]), full[: rank // 2], full[rank // 2 :])
    pl.semaphore_wait(barrier, count - 1)
    for h in range(phases):
        mp_peers(lambda q: copy(slot(FIRST, h), leave.at[FIRST, h, q], land.at[FIRST, h, m], mp=q).start())
    each(early, steps, keep_step)
    each(blocks - blocks // 2, blocks, lambda j: weight_copy(j).start())
    public_copy.start()
    partners_copy.wait()
    sums = []
    for index in range(ROUNDS):
        sums.append(jnp.full((1, lanes), jnp.sum(squares[index]), F32))
        pairs[g, index : index + 1] = jnp.full((1, lanes), partners_ref[index].astype(F32), F32)
    norms[me] = jnp.where(lower(sums[0]), sums[0], sums[1])

    all_peers(lambda p, q: copy(NORM, norms.at[me], norms.at[me], gossip=p, mp=q).start())

    mp_peers(lambda q: copy(GRAM, grams.at[m], grams.at[m], mp=q).start())

    def value_of(kind, j):
        if kind == WEIGHT:
            weight_copy(j).wait()
            return half_ref[0, rows_of(j)].astype(BF16)
        return gv[kind, rows_of(j)]

    def multiply(kind, j):
        product = dot(value_of(kind, j), tall[...])
        h, q = j % phases, wrap(m + j // phases + 1, members)
        if j >= others:
            kept[kind, h] = product
        else:
            leave[kind, h, q] = jnp.stack([pack(product[at : at + step]) for at in range(0, block, step)])
            copy(slot(kind, h), leave.at[kind, h, q], land.at[kind, h, m], mp=q).start()

    for low, high in ((0, others), (others, phases * members)):
        for j in range(low, high):
            with jax.named_scope('second'):
                multiply(SECOND, j)
        for j in range(low, high):
            with jax.named_scope('weight'):
                multiply(WEIGHT, j)
        if low == 0:
            gossip_peers(lambda p: copy(PAIR, pairs.at[g], pairs.at[g], gossip=p).start())

    finish(GRAM, grams.at[pl.ds(0, members - 1)])
    packed = grams[0]
    for index in range(1, members):
        packed = packed + grams[index]
    turned = pltpu.roll(packed, rank, 1)
    gram = jnp.concatenate([jnp.where(lower(packed), packed, turned), jnp.where(lower(packed), turned, packed)], axis=0)
    gram_row = lax.broadcasted_iota(jnp.int32, gram.shape, 0)
    gram_lane = lax.broadcasted_iota(jnp.int32, gram.shape, 1)
    mixer_high, mixer_low = high_low(jnp.where(gram_lane < rank, jnp.where(gram_row == gram_lane, 1.0, 0.0) - gram, 0.0))
    public_copy.wait()
    for h in range(phases):
        at = pl.ds(pl.multiple_of((h * members + m) * block, block), block)
        high, low = high_low(cv[:, at])
        extra[h] = t_dot(high, mixer_high) + t_dot(low, mixer_high) + t_dot(high, mixer_low)

    finish(NORM, norms.at[pl.ds(0, count - 1)])
    norm = jnp.sqrt(jnp.sum(norms[...], axis=0) / total + epsilon)
    turned = pltpu.roll(norm, rank, 1)
    norm = jnp.concatenate([jnp.where(lower(norm), norm, turned), jnp.where(lower(norm), turned, norm)], axis=0)
    scale = step_size * jnp.minimum(1.0, clip_limit / norm)
    scale_0 = scale[0:1]
    scale_1 = scale[1:2]

    for h in range(phases):
        for kind in (FIRST, SECOND, WEIGHT):
            finish(slot(kind, h), land.at[kind, h, pl.ds(0, members - 1)])
        now = kept[WEIGHT, h] - scale_0 * kept[FIRST, h]
        value = jnp.where(lower(now), extra[h] + fold(now), fold(now - scale_1 * kept[SECOND, h]))
        for turn in range(1, members):
            q = wrap(m + turn, members)
            spread = []
            for sub in range(subs):
                first_, second_, weight_ = (land[kind, h, q, sub].astype(F32) for kind in (FIRST, SECOND, WEIGHT))
                now = weight_ - scale_0 * first_
                then = now - scale_1 * second_
                spread.append(jnp.where(lower(now), now, pltpu.roll(then, rank, 1)))
                spread.append(jnp.where(lower(now), pltpu.roll(now, rank, 1), then))
            value = value + jnp.concatenate(spread, axis=0)
        owned[h] = value.reshape(groups, rows, lanes).astype(BF16)
        gossip_peers(lambda p: copy(slot(PIECE, h), owned.at[h, p], first.at[h, g], gossip=p).start())
        first[h, g] = owned[h, g]

    slab = min(16, step)

    factor_0 = scale_0[0, 0]
    factor_1 = scale_1[0, 0]

    def half_step(i):
        at = pl.ds(pl.multiple_of(i * slab, slab), slab)
        half_ref[0, at] = half_ref[0, at] - factor_0 * gv[0, at].astype(F32) - factor_1 * gv[1, at].astype(F32)

    each(0, gv.shape[1] // slab, half_step)

    finish(PAIR, pairs.at[pl.ds(0, groups - 1)])
    inside = lax.broadcasted_iota(jnp.int32, (rows, flat), 0).astype(F32)
    column = lax.broadcasted_iota(jnp.int32, (rows, flat), 1).astype(F32)
    for index in range(ROUNDS):
        blocks = []
        for replica in range(groups):
            wanted = pairs[replica, index : index + 1, 0:1] * float(rows) + inside
            blocks.append(jnp.where(wanted == column, 1.0, 0.0))
        choose[index] = jnp.concatenate(blocks, axis=0).astype(BF16)

    zeros = jnp.zeros((rank, lanes), F32)
    gram_high, gram_low = high_low(jnp.concatenate([gram, zeros], axis=0))
    unit_row = lax.broadcasted_iota(jnp.int32, (lanes, lanes), 0)
    unit_lane = lax.broadcasted_iota(jnp.int32, (lanes, lanes), 1)
    unit = jnp.where(unit_row % rank == unit_lane % rank, 1.0, 0.0).astype(BF16)

    def through(value):
        high, low = high_low(value)
        return dot(high, gram_high) + dot(low, gram_high) + dot(high, gram_low)

    for h in range(phases):
        finish(slot(PIECE, h), first.at[h, pl.ds(0, groups - 1)])
    every = range(phases)
    state = [first[h].astype(F32).reshape(flat, lanes) for h in every]
    narrow = [state[h].astype(BF16) for h in every]
    apart = [dot(choose[0], narrow[h]) - state[h] for h in every]
    again = [(dot(narrow[h], unit) + through(mixing * apart[h] - state[h])).astype(BF16) for h in every]
    sent = [again[h].astype(F32) for h in every]
    later = [dot(choose[1], again[h]) - sent[h] for h in every]
    for h in every:
        answer = jnp.where(lower(sent[h]), mixing * (apart[h] + later[h]), sent[h])
        reply[h] = answer.reshape(groups, rows, lanes).astype(BF16)
    middle = groups // 2
    for h in every:
        def to_all(p):
            for turn in range(members):
                copy(slot(RESULT, h), reply.at[h, p], final.at[h, m * groups + g], gossip=p, mp=wrap(m + turn, members)).start()

        if h < relayed:
            some_peers(1, middle + 1, lambda p: copy(
                slot(FAR, h), reply.at[h, p], final.at[h, m * groups + g], gossip=p).start())
            some_peers(middle + 1, groups, to_all)
        else:
            gossip_peers(to_all)
        mp_peers(lambda q: copy(slot(RESULT, h), reply.at[h, g], final.at[h, m * groups + g], mp=q).start())
        final[h, m * groups + g] = reply[h, g]
    for h in every:
        apart_ref[0, h] = jnp.where(lower(apart[h]), apart[h], 0.0)
        apart_ref[1, h] = jnp.where(lower(later[h]), later[h], 0.0)

    spreads = []
    for index in range(ROUNDS):
        moved = jnp.zeros((), F32)
        for h in range(phases):
            value = apart_ref[index, h]
            moved = moved + jnp.sum(value * through(value))
        spreads.append(jnp.full((1, lanes), moved, F32))
    cons[me] = jnp.where(lower(spreads[0]), spreads[0], spreads[1])
    all_peers(lambda p, q: copy(CONS, cons.at[me], cons.at[me], gossip=p, mp=q).start())
    across = pl.ds(pl.multiple_of(m * groups + jnp.where(g >= middle, 0, middle), middle), middle)
    for h in range(relayed):
        finish(slot(FAR, h), final.at[h, pl.ds(0, middle)])
        mp_peers(lambda q: copy(slot(RELAY, h), final.at[h, across], final.at[h, across], mp=q).start())
    for h in every:
        if h < relayed:
            finish(slot(RELAY, h), final.at[h, pl.ds(0, (members - 1) * middle)])
            finish(slot(RESULT, h), final.at[h, pl.ds(0, members * middle - 1)])
        else:
            finish(slot(RESULT, h), final.at[h, pl.ds(0, count - 1)])
    f_ref[...] = final[...].astype(F32).reshape(f_ref.shape)
    finish(CONS, cons.at[pl.ds(0, count - 1)])
    stat_ref[0] = norm
    drift = jnp.sum(cons[...], axis=0) / total
    turned = pltpu.roll(drift, rank, 1)
    stat_ref[1] = jnp.concatenate([jnp.where(lower(drift), drift, turned), jnp.where(lower(drift), turned, drift)], axis=0)


def blend(h_ref, f_ref, b_ref, stat_ref, out_hbm, c_hbm, drift_hbm, norm_hbm,
          tiles, coefs, drift, norm, stores, others):
    rank, height = coefs.shape
    steps = stores.shape[0]
    step = height // steps

    def store(i):
        at = pl.ds(pl.multiple_of(i * step, step), step)
        return pltpu.make_async_copy(tiles.at[at], out_hbm.at[0, at], stores.at[i])

    def work(i):
        at = pl.ds(pl.multiple_of(i * step, step), step)
        part = f_ref[at, :rank].astype(BF16)
        tiles[at] = h_ref[0, at] + dot(jnp.concatenate([part, part], axis=1), b_ref[...])
        store(i).start()

    each(0, steps, work)
    for index in range(ROUNDS):
        norm[index] = jnp.max(stat_ref[0, index : index + 1, :])
        drift[index] = jnp.max(stat_ref[1, index : index + 1, :])
    coefs[...] = f_ref[...].T[rank:]
    copies = [pltpu.make_async_copy(coefs, c_hbm, others.at[0]), pltpu.make_async_copy(drift, drift_hbm, others.at[1]),
              pltpu.make_async_copy(norm, norm_hbm, others.at[2])]
    for copy in copies:
        copy.start()
    for copy in copies:
        copy.wait()
    each(0, steps, lambda i: store(i).wait())


def body(params, public, gradients, projection, partners):
    groups = lax.axis_size("gossip")
    members = lax.axis_size("mp")
    _, height, columns = params.shape
    rank = projection.shape[1]
    lanes = 2 * rank
    count = groups * members
    total = height * columns * count
    phases = 2 if height % (32 * count) == 0 else 1
    rows = height // (count * phases)
    block = height // (members * phases)
    step = min(128, block)
    subs = block // step
    steps = height // step
    flat = groups * rows
    dma = pltpu.SemaphoreType.DMA
    half, final, basis, stats = pl.pallas_call(
        functools.partial(exchange, groups, members, total),
        in_specs=[HBM] * 5,
        out_specs=[VMEM, VMEM, VMEM, VMEM],
        out_shape=[pltpu.VMEM(params.shape, F32), pltpu.VMEM((height, lanes), F32),
                   pltpu.VMEM((lanes, columns), BF16), pltpu.VMEM((2, ROUNDS, lanes), F32)],
        scratch_shapes=[
            pltpu.VMEM((columns, lanes), BF16),
            pltpu.VMEM((ROUNDS, height, columns), BF16),
            pltpu.VMEM((rank, height), F32),
            pltpu.VMEM((rank, columns), F32),
            pltpu.SMEM((ROUNDS,), jnp.int32),
            pltpu.VMEM((ROUNDS, 8, columns), F32),
            pltpu.VMEM((3, phases, block, lanes), F32),
            pltpu.VMEM((phases, block, lanes), F32),
            pltpu.VMEM((3, phases, members, subs, step // 2, lanes), BF16),
            pltpu.VMEM((3, phases, members, subs, step // 2, lanes), BF16),
            pltpu.VMEM((members, rank // 2, lanes), F32),
            pltpu.VMEM((count, 1, lanes), F32),
            pltpu.VMEM((groups, ROUNDS, lanes), F32),
            pltpu.VMEM((count, 1, lanes), F32),
            pltpu.VMEM((phases, groups, rows, lanes), BF16),
            pltpu.VMEM((phases, groups, rows, lanes), BF16),
            pltpu.VMEM((ROUNDS, flat, flat), BF16),
            pltpu.VMEM((ROUNDS, phases, flat, lanes), F32),
            pltpu.VMEM((phases, groups, rows, lanes), BF16),
            pltpu.VMEM((phases, count, rows, lanes), BF16),
            dma((steps,)), dma((phases * members,)), dma((3,)),
            dma((4 + 7 * phases,)), dma((4 + 7 * phases,)),
        ],
        compiler_params=pltpu.CompilerParams(collective_id=0, has_side_effects=True, vmem_limit_bytes=30 << 20),
        name="exchange",
    )(*[pltpu.with_memory_space_constraint(value, pltpu.HBM) for value in
        (params, gradients, public[0].T, projection.T, partners.reshape(ROUNDS))])

    weights, coefs, drift, norm = pl.pallas_call(
        blend,
        in_specs=[VMEM, VMEM, VMEM, VMEM],
        out_specs=[ANYWHERE, ANYWHERE, ANYWHERE, ANYWHERE],
        out_shape=[jax.ShapeDtypeStruct(params.shape, F32), jax.ShapeDtypeStruct((rank, height), F32),
                   jax.ShapeDtypeStruct((ROUNDS,), F32), jax.ShapeDtypeStruct((ROUNDS,), F32)],
        scratch_shapes=[pltpu.VMEM((height, columns), F32), pltpu.VMEM((rank, height), F32),
                        pltpu.SMEM((ROUNDS,), F32), pltpu.SMEM((ROUNDS,), F32),
                        dma((height // min(128, height),)), dma((3,))],
        compiler_params=pltpu.CompilerParams(vmem_limit_bytes=20 << 20),
        name="blend",
    )(half, final, basis, stats)
    return (weights, coefs.T[None], drift, norm)


def solution(mesh):
    return jax.shard_map(
        body,
        mesh=mesh,
        in_specs=(
            P("gossip", None, "mp"),
            P("gossip", None, None),
            P(None, "gossip", None, "mp"),
            P("mp", None),
            P(None, "gossip"),
        ),
        out_specs=(P("gossip", None, "mp"), P("gossip", None, None), P(), P()),
        check_vma=False,
    )
```

```python
import functools

import jax
import jax.numpy as jnp
from jax import lax
from jax.experimental import pallas as pl
from jax.experimental.pallas import tpu as pltpu
from jax.sharding import PartitionSpec as P

ROUNDS = 2
step_size = 1.0
clip_limit = 0.5
mixing = 0.4
epsilon = 1e-06

F32 = jnp.float32
BF16 = jnp.bfloat16
VMEM = pl.BlockSpec(memory_space=pltpu.VMEM)
HBM = pl.BlockSpec(memory_space=pltpu.HBM)
ANYWHERE = pl.BlockSpec(memory_space=pl.ANY)
MESH = pl.DeviceIdType.MESH


def high_low(value):
    high = value.astype(BF16)
    return high, (value - high.astype(F32)).astype(BF16)


def dot(a, b):
    return jnp.dot(a, b, preferred_element_type=F32)


def dot_t(a, b):
    return lax.dot_general(a, b, (((1,), (1,)), ((), ())), preferred_element_type=F32)


def t_dot(a, b):
    return lax.dot_general(a, b, (((0,), (0,)), ((), ())), preferred_element_type=F32)


def each(low, high, act):
    lax.fori_loop(low, high, lambda i, _: (act(i), 0)[1], 0)


def exchange(groups, members, total, w_hbm, g_hbm, c_hbm, p_hbm, partners_hbm,
             half_ref, f_ref, basis, stat_ref,
             tall, gv, cv, pv, partners_ref, squares, kept, extra, leave, land, grams,
             norms, pairs, cons, owned, first, choose, apart_ref, reply, final,
             load_g, load_w, load_p, send, recv):
    g = lax.axis_index("gossip")
    m = lax.axis_index("mp")
    count = groups * members
    me = g * members + m
    phases, block, lanes = extra.shape
    subs = land.shape[3]
    step = block // subs
    steps = phases * members * subs
    rows = owned.shape[2]
    flat = groups * rows
    rank = lanes // 2
    columns = gv.shape[2]

    def wrap(value, size):
        return jnp.where(value >= size, value - size, value)

    def place(j):
        return j % phases, wrap(m + j // phases + 1, members)

    def span(i):
        h, q = place(i // subs)
        return pl.ds(pl.multiple_of((h * members + q) * block + (i % subs) * step, step), step)

    def grad_copy(i):
        return pltpu.make_async_copy(g_hbm.at[:, 0, span(i)], gv.at[:, span(i)], load_g.at[i])

    def rows_of(j):
        h, q = place(j)
        return pl.ds(pl.multiple_of((h * members + q) * block, block), block)

    def weight_copy(j):
        return pltpu.make_async_copy(w_hbm.at[0, rows_of(j)], half_ref.at[0, rows_of(j)], load_w.at[j])

    basis_copy = pltpu.make_async_copy(p_hbm, pv, load_p.at[0])
    public_copy = pltpu.make_async_copy(c_hbm, cv, load_p.at[1])
    partners_copy = pltpu.make_async_copy(partners_hbm, partners_ref, load_p.at[2])
    basis_copy.start()
    partners_copy.start()
    each(0, steps, lambda i: grad_copy(i).start())

    def partner(k):
        return jnp.bitwise_xor(g, groups - k) if groups & (groups - 1) == 0 else wrap(g + k, groups)

    def some_peers(low, high, act):
        unroll = next(size for size in (5, 4, 3, 2, 1) if (high - low) % size == 0)
        each(0, (high - low) // unroll, lambda j: [act(partner(low + j * unroll + k)) for k in range(unroll)])

    def gossip_peers(act):
        some_peers(1, groups, act)

    def mp_peers(act):
        for turn in range(1, members):
            act(wrap(m + turn, members))

    def all_peers(act):
        gossip_peers(lambda p: [act(p, wrap(m + turn, members)) for turn in range(members)])
        mp_peers(lambda q: act(g, q))

    barrier = pltpu.get_barrier_semaphore()

    def copy(slot, source, target, **device):
        return pltpu.make_async_remote_copy(src_ref=source, dst_ref=target, send_sem=send.at[slot],
                                            recv_sem=recv.at[slot], device_id=device, device_id_type=MESH)

    def finish(slot, ref):
        copy(slot, ref, ref, gossip=wrap(g + 1, groups), mp=m).wait()

    all_peers(lambda p, q: pl.semaphore_signal(barrier, inc=1, device_id={"gossip": p, "mp": q}, device_id_type=MESH))

    NORM, CONS, PAIR, GRAM = range(4)
    FIRST, SECOND, WEIGHT, PIECE, RESULT, FAR, RELAY = range(7)

    def slot(kind, h):
        return 4 + kind * phases + h

    squares[...] = jnp.zeros_like(squares)
    basis_copy.wait()
    high, low = high_low(pv[...])
    basis[...] = jnp.concatenate([high, low], axis=0)
    tall[...] = jnp.concatenate([high.astype(F32), low.astype(F32)], axis=0).T.astype(BF16)

    def fold(value):
        return value + pltpu.roll(value, rank, 1)

    def lower(value):
        return lax.broadcasted_iota(jnp.int32, value.shape, value.ndim - 1) < rank

    def pack(value):
        half = value.shape[0] // 2
        top, bottom = value[:half], value[half:]
        return (jnp.where(lower(top), top, bottom) + pltpu.roll(jnp.where(lower(top), bottom, top), rank, 1)).astype(BF16)

    blocks = phases * members
    lead = blocks // 2 * subs
    others = phases * (members - 1)
    relayed = phases // 2 if groups & (groups - 1) == 0 and members > 1 else 0

    def square_step(i):
        grad_copy(i).wait()

        @pl.when((i >= lead) & (i % subs == 0))
        def _():
            weight_copy((i - lead) // subs).start()

        for index in range(ROUNDS):
            wide = gv[index, span(i)].astype(F32)
            squares[index] += jnp.sum((wide * wide).reshape(step // 8, 8, columns), axis=0)

    def send_step(i):
        square_step(i)
        h, q = place(i // subs)
        leave[FIRST, h, q, i % subs] = pack(dot(gv[0, span(i)], tall[...]))

    def keep_step(i):
        square_step(i)
        h, _ = place(i // subs)
        kept[FIRST, h, pl.ds(pl.multiple_of((i % subs) * step, step), step)] = dot(gv[0, span(i)], tall[...])

    each(0, others * subs, send_step)
    early = max(others * subs, steps * 5 // 8)
    each(others * subs, early, keep_step)
    parts = dot_t(basis[...], basis[...])
    folded = parts + pltpu.roll(parts, rank, 1)
    full = folded[:rank] + folded[rank:]
    grams[m] = jnp.where(lower(full[: rank // 2]), full[: rank // 2], full[rank // 2 :])
    pl.semaphore_wait(barrier, count - 1)
    for h in range(phases):
        mp_peers(lambda q: copy(slot(FIRST, h), leave.at[FIRST, h, q], land.at[FIRST, h, m], mp=q).start())
    each(early, steps, keep_step)
    each(blocks - blocks // 2, blocks, lambda j: weight_copy(j).start())
    public_copy.start()
    partners_copy.wait()
    sums = []
    for index in range(ROUNDS):
        sums.append(jnp.full((1, lanes), jnp.sum(squares[index]), F32))
        pairs[g, index : index + 1] = jnp.full((1, lanes), partners_ref[index].astype(F32), F32)
    norms[me] = jnp.where(lower(sums[0]), sums[0], sums[1])

    all_peers(lambda p, q: copy(NORM, norms.at[me], norms.at[me], gossip=p, mp=q).start())

    mp_peers(lambda q: copy(GRAM, grams.at[m], grams.at[m], mp=q).start())

    def value_of(kind, j):
        if kind == WEIGHT:
            weight_copy(j).wait()
            return half_ref[0, rows_of(j)].astype(BF16)
        return gv[kind, rows_of(j)]

    def multiply(kind, j):
        product = dot(value_of(kind, j), tall[...])
        h, q = j % phases, wrap(m + j // phases + 1, members)
        if j >= others:
            kept[kind, h] = product
        else:
            leave[kind, h, q] = jnp.stack([pack(product[at : at + step]) for at in range(0, block, step)])
            copy(slot(kind, h), leave.at[kind, h, q], land.at[kind, h, m], mp=q).start()

    for low, high in ((0, others), (others, phases * members)):
        for j in range(low, high):
            with jax.named_scope('second'):
                multiply(SECOND, j)
        for j in range(low, high):
            with jax.named_scope('weight'):
                multiply(WEIGHT, j)
        if low == 0:
            gossip_peers(lambda p: copy(PAIR, pairs.at[g], pairs.at[g], gossip=p).start())

    finish(GRAM, grams.at[pl.ds(0, members - 1)])
    packed = grams[0]
    for index in range(1, members):
        packed = packed + grams[index]
    turned = pltpu.roll(packed, rank, 1)
    gram = jnp.concatenate([jnp.where(lower(packed), packed, turned), jnp.where(lower(packed), turned, packed)], axis=0)
    gram_row = lax.broadcasted_iota(jnp.int32, gram.shape, 0)
    gram_lane = lax.broadcasted_iota(jnp.int32, gram.shape, 1)
    mixer_high, mixer_low = high_low(jnp.where(gram_lane < rank, jnp.where(gram_row == gram_lane, 1.0, 0.0) - gram, 0.0))
    public_copy.wait()
    for h in range(phases):
        at = pl.ds(pl.multiple_of((h * members + m) * block, block), block)
        high, low = high_low(cv[:, at])
        extra[h] = t_dot(high, mixer_high) + t_dot(low, mixer_high) + t_dot(high, mixer_low)

    finish(NORM, norms.at[pl.ds(0, count - 1)])
    norm = jnp.sqrt(jnp.sum(norms[...], axis=0) / total + epsilon)
    turned = pltpu.roll(norm, rank, 1)
    norm = jnp.concatenate([jnp.where(lower(norm), norm, turned), jnp.where(lower(norm), turned, norm)], axis=0)
    scale = step_size * jnp.minimum(1.0, clip_limit / norm)
    scale_0 = scale[0:1]
    scale_1 = scale[1:2]

    for h in range(phases):
        for kind in (FIRST, SECOND, WEIGHT):
            finish(slot(kind, h), land.at[kind, h, pl.ds(0, members - 1)])
        now = kept[WEIGHT, h] - scale_0 * kept[FIRST, h]
        value = jnp.where(lower(now), extra[h] + fold(now), fold(now - scale_1 * kept[SECOND, h]))
        for turn in range(1, members):
            q = wrap(m + turn, members)
            spread = []
            for sub in range(subs):
                first_, second_, weight_ = (land[kind, h, q, sub].astype(F32) for kind in (FIRST, SECOND, WEIGHT))
                now = weight_ - scale_0 * first_
                then = now - scale_1 * second_
                spread.append(jnp.where(lower(now), now, pltpu.roll(then, rank, 1)))
                spread.append(jnp.where(lower(now), pltpu.roll(now, rank, 1), then))
            value = value + jnp.concatenate(spread, axis=0)
        owned[h] = value.reshape(groups, rows, lanes).astype(BF16)
        gossip_peers(lambda p: copy(slot(PIECE, h), owned.at[h, p], first.at[h, g], gossip=p).start())
        first[h, g] = owned[h, g]

    slab = min(16, step)

    factor_0 = scale_0[0, 0]
    factor_1 = scale_1[0, 0]

    def half_step(i):
        at = pl.ds(pl.multiple_of(i * slab, slab), slab)
        half_ref[0, at] = half_ref[0, at] - factor_0 * gv[0, at].astype(F32) - factor_1 * gv[1, at].astype(F32)

    each(0, gv.shape[1] // slab, half_step)

    finish(PAIR, pairs.at[pl.ds(0, groups - 1)])
    inside = lax.broadcasted_iota(jnp.int32, (rows, flat), 0).astype(F32)
    column = lax.broadcasted_iota(jnp.int32, (rows, flat), 1).astype(F32)
    for index in range(ROUNDS):
        blocks = []
        for replica in range(groups):
            wanted = pairs[replica, index : index + 1, 0:1] * float(rows) + inside
            blocks.append(jnp.where(wanted == column, 1.0, 0.0))
        choose[index] = jnp.concatenate(blocks, axis=0).astype(BF16)

    zeros = jnp.zeros((rank, lanes), F32)
    gram_high, gram_low = high_low(jnp.concatenate([gram, zeros], axis=0))
    unit_row = lax.broadcasted_iota(jnp.int32, (lanes, lanes), 0)
    unit_lane = lax.broadcasted_iota(jnp.int32, (lanes, lanes), 1)
    unit = jnp.where(unit_row % rank == unit_lane % rank, 1.0, 0.0).astype(BF16)

    def through(value):
        high, low = high_low(value)
        return dot(high, gram_high) + dot(low, gram_high) + dot(high, gram_low)

    for h in range(phases):
        finish(slot(PIECE, h), first.at[h, pl.ds(0, groups - 1)])
    every = range(phases)
    state = [first[h].astype(F32).reshape(flat, lanes) for h in every]
    narrow = [state[h].astype(BF16) for h in every]
    apart = [dot(choose[0], narrow[h]) - state[h] for h in every]
    again = [(dot(narrow[h], unit) + through(mixing * apart[h] - state[h])).astype(BF16) for h in every]
    sent = [again[h].astype(F32) for h in every]
    later = [dot(choose[1], again[h]) - sent[h] for h in every]
    for h in every:
        answer = jnp.where(lower(sent[h]), mixing * (apart[h] + later[h]), sent[h])
        reply[h] = answer.reshape(groups, rows, lanes).astype(BF16)
    middle = groups // 2
    for h in every:
        def to_all(p):
            for turn in reversed(range(members)):
                copy(slot(RESULT, h), reply.at[h, p], final.at[h, m * groups + g], gossip=p, mp=wrap(m + turn, members)).start()

        if h < relayed:
            some_peers(1, middle + 1, lambda p: copy(
                slot(FAR, h), reply.at[h, p], final.at[h, m * groups + g], gossip=p).start())
            some_peers(middle + 1, groups, to_all)
        else:
            gossip_peers(to_all)
        mp_peers(lambda q: copy(slot(RESULT, h), reply.at[h, g], final.at[h, m * groups + g], mp=q).start())
        final[h, m * groups + g] = reply[h, g]
    for h in every:
        apart_ref[0, h] = jnp.where(lower(apart[h]), apart[h], 0.0)
        apart_ref[1, h] = jnp.where(lower(later[h]), later[h], 0.0)

    spreads = []
    for index in range(ROUNDS):
        moved = jnp.zeros((), F32)
        for h in range(phases):
            value = apart_ref[index, h]
            moved = moved + jnp.sum(value * through(value))
        spreads.append(jnp.full((1, lanes), moved, F32))
    cons[me] = jnp.where(lower(spreads[0]), spreads[0], spreads[1])
    all_peers(lambda p, q: copy(CONS, cons.at[me], cons.at[me], gossip=p, mp=q).start())
    across = pl.ds(pl.multiple_of(m * groups + jnp.where(g >= middle, 0, middle), middle), middle)
    for h in range(relayed):
        finish(slot(FAR, h), final.at[h, pl.ds(0, middle)])
        mp_peers(lambda q: copy(slot(RELAY, h), final.at[h, across], final.at[h, across], mp=q).start())
    for h in every:
        if h < relayed:
            finish(slot(RELAY, h), final.at[h, pl.ds(0, (members - 1) * middle)])
            finish(slot(RESULT, h), final.at[h, pl.ds(0, members * middle - 1)])
        else:
            finish(slot(RESULT, h), final.at[h, pl.ds(0, count - 1)])
    f_ref[...] = final[...].astype(F32).reshape(f_ref.shape)
    finish(CONS, cons.at[pl.ds(0, count - 1)])
    stat_ref[0] = norm
    drift = jnp.sum(cons[...], axis=0) / total
    turned = pltpu.roll(drift, rank, 1)
    stat_ref[1] = jnp.concatenate([jnp.where(lower(drift), drift, turned), jnp.where(lower(drift), turned, drift)], axis=0)


def blend(h_ref, f_ref, b_ref, stat_ref, out_hbm, c_hbm, drift_hbm, norm_hbm,
          tiles, coefs, drift, norm, stores, others):
    rank, height = coefs.shape
    steps = stores.shape[0]
    step = height // steps

    def store(i):
        at = pl.ds(pl.multiple_of(i * step, step), step)
        return pltpu.make_async_copy(tiles.at[at], out_hbm.at[0, at], stores.at[i])

    def work(i):
        at = pl.ds(pl.multiple_of(i * step, step), step)
        part = f_ref[at, :rank].astype(BF16)
        tiles[at] = h_ref[0, at] + dot(jnp.concatenate([part, part], axis=1), b_ref[...])
        store(i).start()

    each(0, steps, work)
    for index in range(ROUNDS):
        norm[index] = jnp.max(stat_ref[0, index : index + 1, :])
        drift[index] = jnp.max(stat_ref[1, index : index + 1, :])
    coefs[...] = f_ref[...].T[rank:]
    copies = [pltpu.make_async_copy(coefs, c_hbm, others.at[0]), pltpu.make_async_copy(drift, drift_hbm, others.at[1]),
              pltpu.make_async_copy(norm, norm_hbm, others.at[2])]
    for copy in copies:
        copy.start()
    for copy in copies:
        copy.wait()
    each(0, steps, lambda i: store(i).wait())


def body(params, public, gradients, projection, partners):
    groups = lax.axis_size("gossip")
    members = lax.axis_size("mp")
    _, height, columns = params.shape
    rank = projection.shape[1]
    lanes = 2 * rank
    count = groups * members
    total = height * columns * count
    phases = 2 if height % (32 * count) == 0 else 1
    rows = height // (count * phases)
    block = height // (members * phases)
    step = min(128, block)
    subs = block // step
    steps = height // step
    flat = groups * rows
    dma = pltpu.SemaphoreType.DMA
    half, final, basis, stats = pl.pallas_call(
        functools.partial(exchange, groups, members, total),
        in_specs=[HBM] * 5,
        out_specs=[VMEM, VMEM, VMEM, VMEM],
        out_shape=[pltpu.VMEM(params.shape, F32), pltpu.VMEM((height, lanes), F32),
                   pltpu.VMEM((lanes, columns), BF16), pltpu.VMEM((2, ROUNDS, lanes), F32)],
        scratch_shapes=[
            pltpu.VMEM((columns, lanes), BF16),
            pltpu.VMEM((ROUNDS, height, columns), BF16),
            pltpu.VMEM((rank, height), F32),
            pltpu.VMEM((rank, columns), F32),
            pltpu.SMEM((ROUNDS,), jnp.int32),
            pltpu.VMEM((ROUNDS, 8, columns), F32),
            pltpu.VMEM((3, phases, block, lanes), F32),
            pltpu.VMEM((phases, block, lanes), F32),
            pltpu.VMEM((3, phases, members, subs, step // 2, lanes), BF16),
            pltpu.VMEM((3, phases, members, subs, step // 2, lanes), BF16),
            pltpu.VMEM((members, rank // 2, lanes), F32),
            pltpu.VMEM((count, 1, lanes), F32),
            pltpu.VMEM((groups, ROUNDS, lanes), F32),
            pltpu.VMEM((count, 1, lanes), F32),
            pltpu.VMEM((phases, groups, rows, lanes), BF16),
            pltpu.VMEM((phases, groups, rows, lanes), BF16),
            pltpu.VMEM((ROUNDS, flat, flat), BF16),
            pltpu.VMEM((ROUNDS, phases, flat, lanes), F32),
            pltpu.VMEM((phases, groups, rows, lanes), BF16),
            pltpu.VMEM((phases, count, rows, lanes), BF16),
            dma((steps,)), dma((phases * members,)), dma((3,)),
            dma((4 + 7 * phases,)), dma((4 + 7 * phases,)),
        ],
        compiler_params=pltpu.CompilerParams(collective_id=0, has_side_effects=True, vmem_limit_bytes=30 << 20),
        name="exchange",
    )(*[pltpu.with_memory_space_constraint(value, pltpu.HBM) for value in
        (params, gradients, public[0].T, projection.T, partners.reshape(ROUNDS))])

    weights, coefs, drift, norm = pl.pallas_call(
        blend,
        in_specs=[VMEM, VMEM, VMEM, VMEM],
        out_specs=[ANYWHERE, ANYWHERE, ANYWHERE, ANYWHERE],
        out_shape=[jax.ShapeDtypeStruct(params.shape, F32), jax.ShapeDtypeStruct((rank, height), F32),
                   jax.ShapeDtypeStruct((ROUNDS,), F32), jax.ShapeDtypeStruct((ROUNDS,), F32)],
        scratch_shapes=[pltpu.VMEM((height, columns), F32), pltpu.VMEM((rank, height), F32),
                        pltpu.SMEM((ROUNDS,), F32), pltpu.SMEM((ROUNDS,), F32),
                        dma((height // min(128, height),)), dma((3,))],
        compiler_params=pltpu.CompilerParams(vmem_limit_bytes=20 << 20),
        name="blend",
    )(half, final, basis, stats)
    return (weights, coefs.T[None], drift, norm)


def solution(mesh):
    return jax.shard_map(
        body,
        mesh=mesh,
        in_specs=(
            P("gossip", None, "mp"),
            P("gossip", None, None),
            P(None, "gossip", None, "mp"),
            P("mp", None),
            P(None, "gossip"),
        ),
        out_specs=(P("gossip", None, "mp"), P("gossip", None, None), P(), P()),
        check_vma=False,
    )
```
